32 devices in a mesh: text: 4 (over y, x), graph: 8 (over z, core).
Axes of the slice: x: 2, y: 2, z: 4, core: 2. Of those that a mesh axis runs over, the one named last changes fastest.
Arguments:
- tokens: bfloat16 [16384, 768], P(('text', 'graph')), may hold values from -6 to 6
- doc_ids: int32 [128, 128], P(('text', 'graph')), may hold values from 0 to 3, never falling along the last dimension, each value on 1 to 96 neighbouring positions
- in_gain: float32 [768], replicated, may hold values from 0.25 to 1.75
- in_bias: float32 [768], replicated, may hold values from -3 to 3
- attn_qkv: bfloat16 [768, 2304], P(None, 'text'), may hold values from -0.21875 to 0.21875
- attn_out: bfloat16 [768, 768], P(None, 'text'), may hold values from -0.21875 to 0.21875
- owner_text: int32 [512, 1], P(('text', 'graph')), may hold values from 0 to 3; in each aligned block of 16 rows (0 to 15, 16 to 31, ...) at most 8 rows name the same one
- sage_one: bfloat16 [1536, 768], P('graph'), may hold values from -0.21875 to 0.21875
- sage_two: bfloat16 [1536, 768], P('graph'), may hold values from -0.21875 to 0.21875
- neighbours: int32 [1024, 15], P(('text', 'graph')), may hold values from 0 to 47
- boundary: int32 [256, 2], P(('text', 'graph')), may hold values from 0 to 31
- out_grad: bfloat16 [1024, 768], P(('text', 'graph')), may hold values from -6 to 6
Outputs:
- node_states: bfloat16 [1024, 768], P(('text', 'graph'))
- abstract_grad: bfloat16 [512, 768], P(('text', 'graph'))
The draws below stay inside these ranges and needn't reach their ends.
Inputs may be any that keep to these rules, and one draw needn't show every extreme that they name: `doc_ids`: within each row the numbers never fall; each of the 4 numbers covers 1 to 96 positions. `owner_text`: among the 16 rows of one device no value occurs more than 8 times.
All inputs are finite; a program needn't handle non-finite values.
Results may differ from the reference program's by a relative error of at most 0.01.
Values may be sent and summed in bfloat16 or wider, within the bound.
No kernel may reach another device: no remote copies, remote signals or barrier semaphores. Data moves between devices by JAX's collectives and lax.ppermute only.
A program may use at most 64 MiB of HBM per device.

```python
import math
import jax
import jax.numpy as jnp
import numpy as np
from jax import lax

D = 768
HEAD = 64
HEADS = 12
BLOCK = 128
SEGS = 4
MOST_LEN = 96
BLOCKS = 4
FAN = 15
SLOT = 2
NODE_DEV = 16
TOK_DEV = 512
CAP = 8
ROWS = 32
HALO = 16
ENC_ALL = 512
N_TEXT = 4
N_GRAPH = 8


def plant(result, stream_key, least, largest):
    longest = result.shape.index(max(result.shape))
    spots = []
    for shift in (0, 1):
        where = [jax.random.randint(jax.random.fold_in(stream_key, axis), (), 0, length) for axis, length in enumerate(result.shape)]
        where[longest] = (where[longest] + shift) % result.shape[longest]
        spots.append(tuple(where))
    return result.at[spots[0]].set(least).at[spots[1]].set(largest)


def shard_levels(own_key, shape, cuts, smallest, high):
    gain = 1.0
    for dim, shards_of in cuts:
        draws = jax.random.uniform(jax.random.fold_in(jax.random.fold_in(own_key, 6), dim), (shards_of,), jnp.float32, smallest / len(cuts), high / len(cuts))
        gain = gain * jnp.repeat(jnp.exp(draws), shape[dim] // shards_of).reshape((-1,) + (1,) * (len(shape) - 1 - dim))
    return gain


def profile(amount, total, reach, slope):
    weights = [(1 << 20) // math.isqrt(grade ** slope) + 1 for grade in range(2, amount + 1)]
    rest, holding = total - reach - (amount - 1), [1] * (amount - 1)
    while rest > 0:
        free = [i for i in range(amount - 1) if holding[i] < reach]
        pool, left = sum([weights[i] for i in free]), rest
        for i in free:
            extra = min(reach - holding[i], max(1, left * weights[i] // pool), rest)
            holding[i] = holding[i] + extra
            rest = rest - extra
    return np.array([reach] + holding)


def uneven_parts(key, count, total, bound, skew):
    if count == 2:
        one = jax.random.randint(key, (), max(1, total - bound), min(bound, total - 1) + 1)
        return jnp.stack([one, total - one])
    sizes = jnp.asarray(profile(count, total, bound, skew), jnp.int32)
    pairs = (count - 1) // 2
    source_of, taker = sizes[1:1 + 2 * pairs:2], sizes[2:2 + 2 * pairs:2]
    margin = jnp.minimum(source_of - 1, bound - taker)
    passed = jax.random.randint(jax.random.fold_in(key, 1), (pairs,), 0, 1 << 20) % (margin + 1)
    sizes = sizes.at[1:1 + 2 * pairs:2].set(source_of - passed).at[2:2 + 2 * pairs:2].set(taker + passed)
    return sizes[jax.random.permutation(jax.random.fold_in(key, 2), count)]


def deal_out(rng, own, number, rows, amount, top, bound, skew):
    ranking = jax.random.permutation(rng, amount)
    packed, ordinary = shares(amount, rows * top, bound, skew, True), shares(amount, rows * top, bound, skew, False)
    places = jnp.arange(amount)

    def named(tallies, offset_by):
        used = int((tallies > 0).sum())
        fixed = max(1, used // 4)
        moved = fixed + (places - fixed + offset_by * (used - fixed)) % max(1, amount - fixed)
        return jnp.zeros((amount,), jnp.int32).at[ranking[jnp.where(places < fixed, places, moved)]].set(jnp.asarray(tallies, jnp.int32))

    tallies = jnp.where(number % 4 == 0, named(packed, number // 4), named(ordinary, number - number // 4 - 1))
    mixed = jax.random.permutation(jax.random.fold_in(own, 3), amount)
    donor, taker = mixed[0:amount // 2 * 2:2], mixed[1:amount // 2 * 2:2]
    room = jnp.minimum(tallies[donor] - 1, bound - tallies[taker]) // 2
    room = jnp.where((donor == ranking[0]) | (taker == ranking[0]) | (tallies[taker] == 0), 0, jnp.maximum(room, 0))
    moved = jax.random.randint(jax.random.fold_in(own, 4), (amount // 2,), 0, 1 << 20) % (room + 1)
    tallies = tallies.at[donor].add(-moved).at[taker].add(moved)
    items = jnp.searchsorted(jnp.cumsum(tallies), jnp.arange(rows * top), side="right").astype(jnp.int32)
    listing = items.reshape(top, rows).T
    listing = listing[jax.random.permutation(jax.random.fold_in(own, 1), rows)]
    offset_by = jax.random.randint(jax.random.fold_in(own, 2), (rows, 1), 0, top)
    return jnp.take_along_axis(listing, (jnp.arange(top)[None, :] + offset_by) % top, axis=1)


def shares(number_of, total, reach, skew, full):
    portions = [(1 << 20) // math.isqrt(standing ** skew) + 1 for standing in range(1, number_of + 1)]
    largest = reach if full else min(reach, max(-(-total // number_of), total * portions[0] // sum(portions)))
    least = 1 if total - largest >= number_of - 1 else 0
    holding, surplus = [largest] + [least] * (number_of - 1), total - largest - least * (number_of - 1)
    while surplus > 0:
        movable = [i for i in range(1, number_of) if holding[i] < largest] or [i for i in range(1, number_of) if holding[i] < reach]
        mass, remaining = sum([portions[i] for i in movable]), surplus
        for i in movable:
            more = min(reach - holding[i], max(1, remaining * portions[i] // mass), surplus)
            holding[i] = holding[i] + more
            surplus = surplus - more
    return np.array(holding)


def normal_values(rng, dims, deviation, reach, shards=(), held_as=jnp.bfloat16):
    drawn = deviation * jax.random.normal(rng, dims, jnp.float32)
    if shards:
        drawn = drawn * shard_levels(rng, dims, shards, -0.22, 0.18)
    return jnp.clip(drawn, -reach, reach).astype(held_as)


def setup_inputs(seed: int = 0) -> dict:
    seeds = jax.random.split(jax.random.key(seed), 13)
    tokens = normal_values(seeds[0], (N_TEXT * N_GRAPH * TOK_DEV, D), 1.0, 6.0, ((0, 32),))
    doc_ids = jax.vmap(lambda own: jnp.searchsorted(jnp.cumsum(uneven_parts(own, SEGS, BLOCK, MOST_LEN, 2)), jnp.arange(BLOCK), side="right"))(jax.random.split(seeds[1], (N_TEXT * N_GRAPH * BLOCKS))).reshape((N_TEXT * N_GRAPH * BLOCKS, BLOCK)).astype(jnp.int32)
    in_gain = jnp.clip(1.0 + 0.15 * jax.random.normal(seeds[2], (D,), jnp.float32), 0.25, 1.75)
    in_bias = normal_values(seeds[3], (D,), 0.5, 3.0, (), jnp.float32)
    attn_qkv = normal_values(seeds[4], (D, 3 * D), D ** -0.5, 0.21875, ((1, 4),))
    attn_out = normal_values(seeds[5], (D, D), D ** -0.5, 0.21875, ((1, 4),))
    owner_text_keys = jax.random.split(jax.random.fold_in(seeds[6], 1), ENC_ALL // NODE_DEV)
    owner_text_turns = jax.random.permutation(jax.random.fold_in(seeds[6], 3), ENC_ALL // NODE_DEV)
    owner_text = jax.vmap(lambda own, number: deal_out(jax.random.fold_in(seeds[6], 2), own, number, NODE_DEV, N_TEXT, 1, CAP, 2))(owner_text_keys, owner_text_turns).reshape((ENC_ALL, 1))
    sage_one = normal_values(seeds[7], (2 * D, D), D ** -0.5, 0.21875, ((0, 8),))
    sage_two = normal_values(seeds[8], (2 * D, D), D ** -0.5, 0.21875, ((0, 8),))
    neighbours = plant(jax.random.randint(seeds[9], (N_TEXT * N_GRAPH * ROWS, FAN), 0, ROWS + HALO), jax.random.fold_in(seeds[9], 1), 0, (ROWS + HALO) - 1).astype(jnp.int32)
    boundary = plant(jax.random.randint(seeds[10], (N_TEXT * N_GRAPH * N_GRAPH, SLOT), 0, ROWS), jax.random.fold_in(seeds[10], 1), 0, ROWS - 1).astype(jnp.int32)
    out_grad = normal_values(seeds[11], (N_TEXT * N_GRAPH * ROWS, D), 1.0, 6.0, ((0, 32),))
    return dict(tokens=tokens, doc_ids=doc_ids, in_gain=in_gain, in_bias=in_bias, attn_qkv=attn_qkv, attn_out=attn_out, owner_text=owner_text, sage_one=sage_one, sage_two=sage_two, neighbours=neighbours, boundary=boundary, out_grad=out_grad)


epsilon = 1e-06
highest = lax.Precision.HIGHEST

def encode(device_tokens, device_docs, in_gain, in_bias, attn_qkv, attn_out):
    states = device_tokens.astype(jnp.float32)
    row_mean = lax.optimization_barrier(jnp.mean(states, axis=1, keepdims=True))
    centred = states - row_mean
    variance = lax.optimization_barrier(jnp.mean(centred * centred, axis=1, keepdims=True))
    normed = (centred * lax.rsqrt(variance + epsilon) * in_gain.astype(jnp.float32) + in_bias.astype(jnp.float32)).astype(jnp.bfloat16)
    projected = jnp.dot(normed, attn_qkv, preferred_element_type=jnp.float32).astype(jnp.bfloat16)
    projected = projected.reshape(BLOCKS, BLOCK, 3, HEADS, HEAD).astype(jnp.float32)
    scores = jnp.einsum('bqhd,bkhd->bhqk', projected[:, :, 0], projected[:, :, 1], precision=highest) * HEAD ** (-0.5)
    same_doc = device_docs[:, None, :, None] == device_docs[:, None, None, :]
    weights = jnp.where(same_doc, jnp.exp(scores), 0.0)
    probabilities = (weights / lax.optimization_barrier(jnp.sum(weights, axis=3, keepdims=True))).astype(jnp.bfloat16)
    context = jnp.einsum('bhqk,bkhd->bqhd', probabilities.astype(jnp.float32), projected[:, :, 2], precision=highest)
    context = context.astype(jnp.bfloat16).reshape(TOK_DEV, D)
    node_of = (device_docs + SEGS * jnp.arange(BLOCKS, dtype=jnp.int32)[:, None]).reshape(TOK_DEV)
    member = (node_of[None, :] == jnp.arange(NODE_DEV, dtype=jnp.int32)[:, None]).astype(jnp.float32)
    lengths = lax.optimization_barrier(jnp.sum(member, axis=1, keepdims=True))
    pooled_norm = jnp.dot(member, normed.astype(jnp.float32), precision=highest)
    pooled_context = jnp.dot(member, context.astype(jnp.float32), precision=highest)
    total = pooled_norm + jnp.dot(pooled_context, attn_out.astype(jnp.float32), precision=highest)
    return (total / lengths).astype(jnp.bfloat16)

def slot_table(targets):
    positions = jnp.arange(NODE_DEV, dtype=jnp.int32)
    earlier = (positions[None, :] < positions[:, None]) & (targets[None, :] == targets[:, None])
    slot_index = targets.astype(jnp.int32) * CAP + lax.optimization_barrier(jnp.sum(earlier.astype(jnp.int32), axis=1)).astype(jnp.int32)
    return (slot_index[:, None] == jnp.arange(ROWS, dtype=jnp.int32)[None, :]).astype(jnp.float32)

def reference(tokens, doc_ids, in_gain, in_bias, attn_qkv, attn_out, owner_text, sage_one, sage_two, neighbours, boundary, out_grad):
    devices = N_TEXT * N_GRAPH
    embedded = lax.map(lambda arrays: encode(arrays[0], arrays[1], in_gain, in_bias, attn_qkv, attn_out), (tokens.reshape(devices, TOK_DEV, D), doc_ids.reshape(devices, BLOCKS, BLOCK)))
    slots = jax.vmap(slot_table)(owner_text.reshape(devices, NODE_DEV))
    outgoing = jnp.einsum('dnr,dnc->drc', slots, embedded.astype(jnp.float32), precision=highest)
    filled = lax.optimization_barrier(jnp.sum(slots, axis=1))
    arrived = outgoing.reshape(N_TEXT, N_GRAPH, N_TEXT, CAP, D).transpose(2, 1, 0, 3, 4).reshape(devices, ROWS, D).astype(jnp.bfloat16)
    live_rows = filled.reshape(N_TEXT, N_GRAPH, N_TEXT, CAP).transpose(2, 1, 0, 3).reshape(devices, ROWS, 1)
    extent = ROWS + HALO
    adjacency = lax.optimization_barrier(jnp.sum((neighbours.reshape(devices, ROWS, FAN, 1) == jnp.arange(extent, dtype=jnp.int32)).astype(jnp.float32), axis=2))
    picker = (boundary.reshape(devices, HALO, 1) == jnp.arange(ROWS, dtype=jnp.int32)).astype(jnp.float32)

    def trade(hidden):
        leaving = jnp.einsum('dhr,drc->dhc', picker, hidden.astype(jnp.float32), precision=highest)
        leaving = leaving.reshape(N_TEXT, N_GRAPH, N_GRAPH, SLOT, D).transpose(0, 2, 1, 3, 4)
        return leaving.reshape(devices, HALO, D).astype(jnp.bfloat16)

    def give_back(halo_grad):
        moved = halo_grad.astype(jnp.float32).reshape(N_TEXT, N_GRAPH, N_GRAPH, SLOT, D).transpose(0, 2, 1, 3, 4)
        return jnp.einsum('dhr,dhc->drc', picker, moved.reshape(devices, HALO, D), precision=highest)

    def forward_layer(hidden, weight):
        extended = jnp.concatenate([hidden, trade(hidden)], axis=1).astype(jnp.float32)
        aggregated = (jnp.einsum('dre,dec->drc', adjacency, extended, precision=highest) / FAN).astype(jnp.bfloat16)
        wide_weight = weight.astype(jnp.float32)
        return jnp.einsum('drc,ce->dre', hidden.astype(jnp.float32), wide_weight[:D], precision=highest) + jnp.einsum('drc,ce->dre', aggregated.astype(jnp.float32), wide_weight[D:], precision=highest)

    def backward_layer(gradient, weight):
        wide_weight = weight.astype(jnp.float32)
        wide_gradient = gradient.astype(jnp.float32)
        self_part = jnp.einsum('dre,ce->drc', wide_gradient, wide_weight[:D], precision=highest)
        spread = (jnp.einsum('dre,ce->drc', wide_gradient, wide_weight[D:], precision=highest) / FAN).astype(jnp.bfloat16)
        ext_grad = jnp.einsum('dre,drc->dec', adjacency, spread.astype(jnp.float32), precision=highest)
        return self_part + ext_grad[:, :ROWS] + give_back(ext_grad[:, ROWS:].astype(jnp.bfloat16))
    preact_one = forward_layer(arrived, sage_one)
    hidden_one = (live_rows * jax.nn.gelu(preact_one)).astype(jnp.bfloat16)
    preact_two = forward_layer(hidden_one, sage_two)
    node_states = (live_rows * preact_two).astype(jnp.bfloat16)
    grad_two = (live_rows * out_grad.reshape(devices, ROWS, D).astype(jnp.float32)).astype(jnp.bfloat16)
    into_one = backward_layer(grad_two, sage_two)
    gelu_value, pull_back = jax.vjp(jax.nn.gelu, preact_one)
    grad_one = (live_rows * pull_back(into_one)[0]).astype(jnp.bfloat16)
    embed_grad = backward_layer(grad_one, sage_one).astype(jnp.bfloat16)
    returned = embed_grad.astype(jnp.float32).reshape(N_TEXT, N_GRAPH, N_TEXT, CAP, D).transpose(2, 1, 0, 3, 4).reshape(devices, ROWS, D)
    abstract_grad = jnp.einsum('dnr,drc->dnc', slots, returned, precision=highest).astype(jnp.bfloat16)
    return (node_states.reshape(devices * ROWS, D), abstract_grad.reshape(ENC_ALL, D))
```

```python
import jax
import jax.numpy as jnp
from jax import lax
from jax.sharding import PartitionSpec as P

HEAD = 64
SEGS = 4
CORES = 2


epsilon = 1e-06
bf16 = jnp.bfloat16
f32 = jnp.float32


def dot(left, right, contract, batch=((), ())):
    return lax.dot_general(left, right, (contract, batch), preferred_element_type=f32)


def over_text(array, step):
    count = lax.axis_size("text")
    return lax.ppermute(array, "text", [(i, i ^ step) for i in range(count)])


def over_graph(array, step):
    count = lax.axis_size("graph")
    return lax.ppermute(array, "graph", [(i, i ^ step) for i in range(count)])


def over_pair(array, steps):
    texts, graphs = lax.axis_size("text"), lax.axis_size("graph")
    moves = []
    for t in range(texts):
        for g in range(graphs):
            moves.append((t * graphs + g, (t ^ steps[g % CORES]) * graphs + g))
    return lax.ppermute(array, ("text", "graph"), moves)


def natural(parts, own):
    stacked = jnp.stack(parts)
    return jnp.concatenate(
        [lax.dynamic_index_in_dim(stacked, own ^ j, 0, keepdims=True) for j in range(len(parts))]
    )


def gather_text(shard, text, core):
    count = lax.axis_size("text")
    half = shard.shape[1] // CORES
    first = [over_pair(shard, (k, k + 1)) for k in range(1, count - 1, 2)]
    split = lax.dynamic_slice_in_dim(shard, core * half, half, 1)
    last = over_text(split, count - 1)
    parts = [shard]
    for got in first:
        swapped = over_graph(got, 1)
        parts.append(jnp.where(core == 0, got, swapped))
        parts.append(jnp.where(core == 0, swapped, got))
    swapped = over_graph(last, 1)
    parts.append(
        jnp.concatenate(
            [jnp.where(core == 0, last, swapped), jnp.where(core == 0, swapped, last)], axis=1
        )
    )
    return natural(parts, text)


def gather_graph(array):
    count = lax.axis_size("graph")
    mine = jnp.stack([array] + [over_graph(array, k) for k in range(CORES, count, CORES)])
    return jnp.stack([mine, over_graph(mine, 1)], axis=1).reshape((count,) + array.shape)


def encode(tokens, doc_ids, in_gain, in_bias, qkv, out_proj):
    width = tokens.shape[1]
    blocks, block_len = doc_ids.shape
    head_count = width // HEAD
    states = tokens.astype(f32)
    row_mean = jnp.mean(states, axis=1, keepdims=True)
    centred = states - row_mean
    variance = jnp.mean(centred * centred, axis=1, keepdims=True)
    normed = (centred * lax.rsqrt(variance + epsilon) * in_gain + in_bias).astype(bf16)
    projected = dot(normed, qkv, ((1,), (1,))).astype(bf16)
    projected = projected.reshape(blocks, block_len, 3, head_count, HEAD)
    scores = jnp.einsum(
        "bqhd,bkhd->bhqk", projected[:, :, 0], projected[:, :, 1], preferred_element_type=f32
    ) * HEAD ** (-0.5)
    same_doc = doc_ids[:, None, :, None] == doc_ids[:, None, None, :]
    weights = jnp.where(same_doc, jnp.exp(scores), 0.0)
    probabilities = (weights / jnp.sum(weights, axis=3, keepdims=True)).astype(bf16)
    context = jnp.einsum(
        "bhqk,bkhd->bqhd", probabilities, projected[:, :, 2], preferred_element_type=f32
    )
    context = context.astype(bf16).reshape(blocks * block_len, width)
    node_total = blocks * SEGS
    node_of = (doc_ids + SEGS * jnp.arange(blocks, dtype=jnp.int32)[:, None]).reshape(-1)
    member = (node_of[None, :] == jnp.arange(node_total, dtype=jnp.int32)[:, None]).astype(bf16)
    lengths = jnp.sum(member.astype(f32), axis=1, keepdims=True)
    pooled_norm = dot(member, normed, ((1,), (0,)))
    pooled_context = (dot(member, context, ((1,), (0,))) / lengths).astype(bf16)
    return (pooled_norm / lengths + dot(pooled_context, out_proj, ((1,), (1,)))).astype(bf16)


def local(
    tokens,
    doc_ids,
    in_gain,
    in_bias,
    attn_qkv,
    attn_out,
    owner_text,
    sage_one,
    sage_two,
    neighbours,
    boundary,
    out_grad,
):
    width = tokens.shape[1]
    texts, graphs = lax.axis_size("text"), lax.axis_size("graph")
    text, graph = lax.axis_index("text"), lax.axis_index("graph")
    core, z = graph % CORES, graph // CORES
    rows = out_grad.shape[0]
    made = owner_text.shape[0]
    capacity = rows // texts
    fan = neighbours.shape[1]
    slot_count = boundary.shape[1]
    i32 = jnp.int32

    qkv = gather_text(attn_qkv.T, text, core).reshape(-1, width)
    out_proj = gather_text(attn_out.T, text, core).reshape(-1, width)

    depth = sage_one.shape[0]
    share = depth // texts
    hidden = (graphs // 2) * share
    lanes = next(n for n in range(128, width + 1, 128) if n >= hidden and width % n == 0)
    column = jnp.arange(lanes, dtype=i32)
    wanted = (column // share) * depth + text * share + column % share
    wanted = jnp.where(column < hidden, wanted, -1)
    chosen = (jnp.arange(width, dtype=i32)[:, None] == wanted[None, :]).astype(bf16)
    one_share = dot(sage_one, chosen, ((1,), (0,))).astype(bf16)
    two_share = lax.dynamic_slice_in_dim(sage_two, text * share, share, 0)
    packed = jnp.concatenate(
        [one_share] + [two_share[:, i : i + lanes] for i in range(0, width, lanes)], axis=0
    )
    got = gather_graph(packed)
    got = natural(
        [got[CORES * k : CORES * (k + 1)] for k in range(graphs // CORES)], z
    )
    got = jnp.where(core == 0, got, got[:, ::-1]).reshape(graphs, -1, lanes)
    one = got[:, :depth].reshape(2, width, lanes)
    two = got[:, depth:].reshape(2, hidden // share, width // lanes, share, lanes)
    two = two.transpose(0, 1, 3, 2, 4).reshape(2, hidden, width)
    one = one[:, :, :hidden]

    facts = jnp.concatenate(
        [neighbours.reshape(-1), boundary.reshape(-1), owner_text.reshape(-1)]
    ).astype(bf16)
    fact_count = facts.shape[0]
    fact_rows = -(-fact_count // width)
    facts = jnp.pad(facts, (0, fact_rows * width - fact_count)).reshape(fact_rows, width)
    outset = jnp.concatenate([out_grad, facts], axis=0)
    outset = jnp.stack([outset] + [over_text(outset, k) for k in range(1, texts)])
    grads = outset[:, :rows]
    facts = outset[:, rows:].reshape(texts, -1)[:, :fact_count]

    def slot_places(owners):
        same = owners[..., :, None] == owners[..., None, :]
        order = jnp.arange(made, dtype=i32)
        earlier = jnp.sum((same & (order[None, :] < order[:, None])).astype(i32), axis=-1)
        source = text ^ jnp.arange(texts, dtype=i32)
        place = (owners ^ text) * rows + source[:, None] * capacity + earlier
        return place.reshape(owners.shape[:-2] + (1, texts * made))

    own_places = slot_places(facts[:, fact_count - made :].astype(i32))
    own_table = (own_places == jnp.arange(texts * rows, dtype=i32)[:, None]).astype(bf16)
    live_grad = dot(own_table, grads.reshape(texts * rows, width), ((0,), (0,))).astype(bf16)
    up = jnp.concatenate(
        [dot(live_grad, two[0], ((1,), (1,))), dot(live_grad, two[1], ((1,), (1,)))], axis=1
    ).astype(bf16)
    wide = 2 * hidden
    all_count = texts * fact_count
    all_rows = -(-all_count // wide)
    flat = jnp.pad(facts.reshape(-1), (0, all_rows * wide - all_count)).reshape(all_rows, wide)
    shared = gather_graph(jnp.concatenate([up, flat], axis=0))
    ups = shared[:, : texts * made]
    facts = shared[:, texts * made :].reshape(graphs, -1)[:, :all_count]
    facts = facts.reshape(graphs, texts, fact_count).astype(i32)

    listed = facts[..., : rows * fan].reshape(graphs, texts, rows, fan)
    bounds = facts[..., rows * fan : fact_count - made].reshape(graphs, texts, graphs, slot_count)
    owners = facts[..., fact_count - made :]
    places = slot_places(owners)
    peer = graph ^ jnp.arange(graphs, dtype=i32)
    halo_name = (rows + peer[:, None] * slot_count + jnp.arange(slot_count, dtype=i32)).reshape(-1)
    extended_name = jnp.concatenate([jnp.arange(rows, dtype=i32), halo_name])
    turned = (jnp.arange(graphs, dtype=i32)[:, None] == peer[None, :]).astype(f32)
    halo_row = jnp.einsum("ptgk,gd->tdpk", bounds.astype(f32), turned).astype(i32)
    halo_row = halo_row.reshape(texts, graphs, graphs * slot_count)
    halo_at = jnp.repeat(jnp.arange(graphs, dtype=i32), slot_count) * rows + halo_row
    nodes = graphs * rows

    def node_stage(one_text):
        distance, listed, halo_at = one_text
        counts = jnp.sum((listed[..., None] == extended_name).astype(f32), axis=2).astype(bf16)
        table = (places == distance * rows + jnp.arange(rows, dtype=i32)[:, None]).astype(bf16)
        live = jnp.sum(table.astype(f32), axis=2).reshape(nodes, 1)

        def to_rows(by_abstract):
            return dot(table, by_abstract, ((2,), (1,)), ((0,), (0,))).reshape(nodes, -1)

        if dense:
            self_at = jnp.arange(nodes, dtype=i32).reshape(graphs, rows)
            at = jnp.concatenate([self_at, halo_at], axis=1)
            place = (at[..., None] == jnp.arange(nodes, dtype=i32)).astype(bf16)
            links = dot(counts, place, ((2,), (1,)), ((0,), (0,)))
            links = links.astype(bf16).reshape(nodes, nodes)

            def pull(values, count):
                return dot(links[:count], values, ((1,), (0,)))

            def push(values, count):
                return dot(links[:, :count], values, ((0,), (0,)))

        else:
            halo = halo_at.reshape(-1)

            def pull(values, count):
                outer = values[halo].reshape(graphs, -1, values.shape[1])
                inner = values.reshape(graphs, rows, -1)
                extended = jnp.concatenate([inner, outer], axis=1)
                out = dot(counts, extended, ((2,), (1,)), ((0,), (0,)))
                return out.reshape(nodes, -1)[:count]

            def push(values, count):
                out = dot(counts, values.reshape(graphs, rows, -1), ((1,), (1,)), ((0,), (0,)))
                inner = out[:, :rows].reshape(nodes, -1)
                return inner.at[halo].add(out[:, rows:].reshape(halo.shape[0], -1))[:count]

        up_rows = to_rows(ups)
        into_one = up_rows[:, :hidden] + push(up_rows[:, hidden:].astype(bf16), nodes) / fan
        first_rows = to_rows(firsts)
        preact_one = first_rows[:, :hidden] + pull(first_rows[:, hidden:].astype(bf16), nodes) / fan
        gelu_value, pull_back = jax.vjp(jax.nn.gelu, preact_one)
        hidden_one = (live * gelu_value).astype(bf16)
        grad_one = (live * pull_back(into_one)[0]).astype(bf16)
        aggregated = (pull(hidden_one, rows) / fan).astype(bf16)
        returned = (push(grad_one, rows) / fan).astype(bf16)
        return (
            jnp.concatenate([hidden_one[:rows], aggregated], axis=1),
            jnp.concatenate([grad_one[:rows], returned], axis=1),
            live[:rows],
        )

    embedded = encode(tokens, doc_ids, in_gain, in_bias, qkv, out_proj)
    gathered = jnp.concatenate(
        [embedded] + [over_text(embedded, k) for k in range(1, texts)], axis=0
    )
    first = jnp.concatenate(
        [dot(gathered, one[0], ((1,), (0,))), dot(gathered, one[1], ((1,), (0,)))], axis=1
    ).astype(bf16)
    firsts = gather_graph(first)

    dense = texts * graphs <= 64
    per_text = (jnp.arange(texts, dtype=i32), listed.transpose(1, 0, 2, 3), halo_at)
    if dense:
        forth, back, live = jax.vmap(node_stage)(per_text)
    else:
        forth, back, live = lax.map(node_stage, per_text)
    forth = forth.reshape(texts * rows, wide)
    state_part = dot(forth[:, :hidden], two[0], ((1,), (0,))) + dot(
        forth[:, hidden:], two[1], ((1,), (0,))
    )
    back = dot(own_table, back.reshape(texts * rows, wide), ((0,), (0,))).astype(bf16)
    grad_part = dot(back[:, :hidden], one[0], ((1,), (1,))) + dot(
        back[:, hidden:], one[1], ((1,), (1,))
    )

    final = jnp.concatenate(
        [state_part.reshape(texts, rows, width), grad_part.reshape(texts, made, width)], axis=1
    )
    total = final[0]
    outgoing = final.astype(bf16)
    for k in range(1, texts):
        total = total + over_text(outgoing[k], k).astype(f32)
    node_states = (live[0] * total[:rows]).astype(bf16)
    return (node_states, total[rows:].astype(bf16))


def solution(mesh):
    rowwise = P(("text", "graph"), None)
    placed = (
        rowwise,
        rowwise,
        P(),
        P(),
        P(None, "text"),
        P(None, "text"),
        rowwise,
        P("graph", None),
        P("graph", None),
        rowwise,
        rowwise,
        rowwise,
    )
    return jax.shard_map(
        local, mesh=mesh, in_specs=placed, out_specs=(rowwise, rowwise), check_vma=False
    )
```

```python
import jax
import jax.numpy as jnp
from jax import lax
from jax.experimental import pallas as pl
from jax.experimental.pallas import tpu as pltpu
from jax.sharding import PartitionSpec as P

HEAD = 64
SEGS = 4
CORES = 2


epsilon = 1e-06
bf16 = jnp.bfloat16
f32 = jnp.float32


def dot(left, right, contract, batch=((), ())):
    return lax.dot_general(left, right, (contract, batch), preferred_element_type=f32)


def over_text(array, step):
    count = lax.axis_size("text")
    return lax.ppermute(array, "text", [(i, i ^ step) for i in range(count)])


def over_graph(array, step):
    count = lax.axis_size("graph")
    return lax.ppermute(array, "graph", [(i, i ^ step) for i in range(count)])


def over_pair(array, steps):
    texts, graphs = lax.axis_size("text"), lax.axis_size("graph")
    moves = []
    for t in range(texts):
        for g in range(graphs):
            moves.append((t * graphs + g, (t ^ steps[g % CORES]) * graphs + g))
    return lax.ppermute(array, ("text", "graph"), moves)


def natural(parts, own):
    stacked = jnp.stack(parts)
    return jnp.concatenate(
        [lax.dynamic_index_in_dim(stacked, own ^ j, 0, keepdims=True) for j in range(len(parts))]
    )


def fetch_text(shard, core):
    count = lax.axis_size("text")
    half = shard.shape[1] // CORES
    whole = [over_pair(shard, (k, k + 1)) for k in range(1, count - 1, 2)]
    split = lax.dynamic_slice_in_dim(shard, core * half, half, 1)
    return whole + [over_text(split, count - 1)]


def pieces_of(shard, fetched):
    return [shard] + [piece for got in fetched for piece in (got, over_graph(got, 1))]


def place_pieces(refs, whole, sem):
    text, core = lax.axis_index("text"), lax.axis_index("graph") % CORES
    rows, width = refs[0].shape
    count = whole.shape[0] // rows
    half = width // CORES
    spots = [(text, 0, width)]
    for k in range(1, count - 1, 2):
        spots += [(text ^ (k + core), 0, width), (text ^ (k + 1 - core), 0, width)]
    spots += [(text ^ (count - 1), core * half, half), (text ^ (count - 1), (1 - core) * half, half)]
    copies = []
    for i, (ref, (peer, lane, lanes)) in enumerate(zip(refs, spots)):
        at = pl.ds(pl.multiple_of(peer * rows, rows), rows)
        if lanes == width:
            target = whole.at[at, :]
        else:
            target = whole.at[at, pl.ds(pl.multiple_of(lane, half), half)]
        copies.append(pltpu.make_async_copy(ref, target, sem.at[i]))
    return copies


def assemble(pieces, text, core):
    parts = [pieces[0]]
    for got, swapped in zip(pieces[1:-2:2], pieces[2:-2:2]):
        parts.append(jnp.where(core == 0, got, swapped))
        parts.append(jnp.where(core == 0, swapped, got))
    got, swapped = pieces[-2:]
    parts.append(
        jnp.concatenate(
            [jnp.where(core == 0, got, swapped), jnp.where(core == 0, swapped, got)], axis=1
        )
    )
    return natural(parts, text).reshape(-1, parts[0].shape[1])


def gather_graph(array):
    count = lax.axis_size("graph")
    mine = jnp.stack([array] + [over_graph(array, k) for k in range(CORES, count, CORES)])
    return jnp.stack([mine, over_graph(mine, 1)], axis=1).reshape((count,) + array.shape)


def layer_norm(tokens, in_gain, in_bias):
    states = tokens.astype(f32)
    row_mean = jnp.mean(states, axis=1, keepdims=True)
    centred = states - row_mean
    variance = jnp.mean(centred * centred, axis=1, keepdims=True)
    return (centred * lax.rsqrt(variance + epsilon) * in_gain + in_bias).astype(bf16)


def attention_kernel(*refs):
    normed_ref, doc_ref, doc_column_ref = refs[:3]
    norm_out, context_out, weights, projected, raised, sem = refs[-6:]
    copies = place_pieces(refs[3:-6], weights, sem)
    for copy in copies:
        copy.start()
    width = normed_ref.shape[1]
    blocks, length = doc_ref.shape
    pair = 2 * HEAD
    lane = lax.broadcasted_iota(jnp.int32, (2 * length, pair), 1)
    row = lax.broadcasted_iota(jnp.int32, (2 * length, pair), 0)
    own_half = (lane < HEAD) == (row < length)
    scale = jnp.where(own_half, HEAD ** (-0.5), 0.0).astype(bf16)
    ones = jnp.ones((2 * SEGS, pair), bf16)
    own_head = (lax.broadcasted_iota(jnp.int32, (4 * SEGS, 2 * length), 0) < 2 * SEGS) == (
        lax.broadcasted_iota(jnp.int32, (4 * SEGS, 2 * length), 1) < length
    )
    members = []
    lengths = []
    for b in range(blocks):
        number = lax.broadcasted_iota(jnp.int32, (2 * SEGS, length), 0)
        member = jnp.where(doc_ref[b : b + 1, :] == number, 1.0, 0.0)
        count = jnp.sum(member, axis=1, keepdims=True)[:SEGS]
        members.append(jnp.concatenate([member, member]))
        lengths.append(count)
        at = slice(b * length, (b + 1) * length)
        pooled = dot(member.astype(bf16), normed_ref[at, :], ((1,), (0,)))
        norm_out[b * SEGS : (b + 1) * SEGS, :] = pooled[:SEGS] / count
    for copy in copies:
        copy.wait()
    step = 2 * pair
    for n in range(0, 3 * width, step):
        out = dot(normed_ref[...], weights[n : n + step, :], ((1,), (1,)))
        projected[:, n : n + step] = out.astype(bf16)
    for b in range(blocks):
        at = slice(b * length, (b + 1) * length)
        same = doc_column_ref[:, b : b + 1] == doc_ref[b : b + 1, :]
        same = jnp.concatenate([same, same])
        starts = range(0, width, pair)
        for i, n in enumerate(starts):
            queries = projected[at, n : n + pair]
            keys = projected[at, width + n : width + n + pair]
            scores = dot(jnp.concatenate([queries, queries]) * scale, keys, ((1,), (1,)))
            raised[i] = jnp.where(same, jnp.exp(scores), 0.0).astype(bf16)
        totals = [dot(ones, raised[i], ((1,), (1,))) for i, n in enumerate(starts)]
        shares = []
        for i, n in enumerate(starts):
            inverse = 1.0 / totals[i]
            inverse = jnp.where(own_head, jnp.concatenate([inverse, inverse]), 0.0)
            high = inverse.astype(bf16)
            low = (inverse - high.astype(f32)).astype(bf16)
            both = dot(jnp.concatenate([high, low]), raised[i], ((1,), (0,)))
            shares.append(both[: 4 * SEGS] + both[4 * SEGS :])
        for i, n in enumerate(starts):
            values = projected[at, 2 * width + n : 2 * width + n + pair]
            mixed = dot((members[b] * shares[i]).astype(bf16), values, ((1,), (0,)))
            both = jnp.where(lane[: 2 * SEGS] < HEAD, mixed[: 2 * SEGS], mixed[2 * SEGS :])
            context_out[b * SEGS : (b + 1) * SEGS, n : n + pair] = both[:SEGS] / lengths[b]


def attention(normed, doc_ids, pieces):
    tokens, width = normed.shape
    blocks, length = doc_ids.shape
    vmem, anywhere = pl.BlockSpec(memory_space=pltpu.VMEM), pl.BlockSpec(memory_space=pl.ANY)
    pooled = jax.ShapeDtypeStruct((blocks * SEGS, width), f32)
    flops = 2 * tokens * width * 3 * width + 6 * tokens * length * width
    return pl.pallas_call(
        attention_kernel,
        out_shape=(pooled, pooled),
        in_specs=[vmem] * 3 + [anywhere] * len(pieces),
        out_specs=(vmem, vmem),
        scratch_shapes=[
            pltpu.VMEM((3 * width, width), bf16),
            pltpu.VMEM((tokens, 3 * width), bf16),
            pltpu.VMEM((width // (2 * HEAD), 2 * length, length), bf16),
            pltpu.SemaphoreType.DMA((len(pieces),)),
        ],
        cost_estimate=pl.CostEstimate(
            flops=flops, bytes_accessed=8 * width * width, transcendentals=tokens * length * width // HEAD
        ),
        name="attention",
    )(normed, doc_ids, doc_ids.T, *pieces)


def local(
    tokens,
    doc_ids,
    in_gain,
    in_bias,
    attn_qkv,
    attn_out,
    owner_text,
    sage_one,
    sage_two,
    neighbours,
    boundary,
    out_grad,
):
    width = tokens.shape[1]
    texts, graphs = lax.axis_size("text"), lax.axis_size("graph")
    text, graph = lax.axis_index("text"), lax.axis_index("graph")
    core, z = graph % CORES, graph // CORES
    rows = out_grad.shape[0]
    made = owner_text.shape[0]
    capacity = rows // texts
    fan = neighbours.shape[1]
    slot_count = boundary.shape[1]
    i32 = jnp.int32

    qkv_shard, out_shard = attn_qkv.T, attn_out.T
    qkv_fetched = fetch_text(qkv_shard, core)
    out_fetched = fetch_text(out_shard, core)
    qkv_pieces = pieces_of(qkv_shard, qkv_fetched)
    out_pieces = pieces_of(out_shard, out_fetched)

    depth = sage_one.shape[0]
    share = depth // texts
    hidden = (graphs // 2) * share
    lanes = next(n for n in range(128, width + 1, 128) if n >= hidden and width % n == 0)
    column = jnp.arange(lanes, dtype=i32)
    wanted = (column // share) * depth + text * share + column % share
    wanted = jnp.where(column < hidden, wanted, -1)
    chosen = (jnp.arange(width, dtype=i32)[:, None] == wanted[None, :]).astype(bf16)
    one_share = dot(sage_one, chosen, ((1,), (0,))).astype(bf16)
    two_share = lax.dynamic_slice_in_dim(sage_two, text * share, share, 0)
    packed = jnp.concatenate(
        [one_share] + [two_share[:, i : i + lanes] for i in range(0, width, lanes)], axis=0
    )
    got = gather_graph(packed)
    got = natural(
        [got[CORES * k : CORES * (k + 1)] for k in range(graphs // CORES)], z
    )
    got = jnp.where(core == 0, got, got[:, ::-1]).reshape(graphs, -1, lanes)
    one = got[:, :depth].reshape(2, width, lanes)
    two = got[:, depth:].reshape(2, hidden // share, width // lanes, share, lanes)
    two = two.transpose(0, 1, 3, 2, 4).reshape(2, hidden, width)
    one = one[:, :, :hidden]

    facts = jnp.concatenate(
        [neighbours.reshape(-1), boundary.reshape(-1), owner_text.reshape(-1)]
    ).astype(bf16)
    fact_count = facts.shape[0]
    fact_rows = -(-fact_count // width)
    facts = jnp.pad(facts, (0, fact_rows * width - fact_count)).reshape(fact_rows, width)
    outset = jnp.concatenate([out_grad, facts], axis=0)
    outset = jnp.stack([outset] + [over_text(outset, k) for k in range(1, texts)])
    grads = outset[:, :rows]
    facts = outset[:, rows:].reshape(texts, -1)[:, :fact_count]

    def slot_places(owners):
        same = owners[..., :, None] == owners[..., None, :]
        order = jnp.arange(made, dtype=i32)
        earlier = jnp.sum((same & (order[None, :] < order[:, None])).astype(i32), axis=-1)
        source = text ^ jnp.arange(texts, dtype=i32)
        place = (owners ^ text) * rows + source[:, None] * capacity + earlier
        return place.reshape(owners.shape[:-2] + (1, texts * made))

    own_places = slot_places(facts[:, fact_count - made :].astype(i32))
    own_table = (own_places == jnp.arange(texts * rows, dtype=i32)[:, None]).astype(bf16)
    wide = 2 * hidden
    all_count = texts * fact_count
    all_rows = -(-all_count // width)
    flat = jnp.pad(facts.reshape(-1), (0, all_rows * width - all_count)).reshape(all_rows, width)
    facts = gather_graph(flat).reshape(graphs, -1)[:, :all_count]
    facts = facts.reshape(graphs, texts, fact_count).astype(i32)

    listed = facts[..., : rows * fan].reshape(graphs, texts, rows, fan)
    bounds = facts[..., rows * fan : fact_count - made].reshape(graphs, texts, graphs, slot_count)
    owners = facts[..., fact_count - made :]
    places = slot_places(owners)
    peer = graph ^ jnp.arange(graphs, dtype=i32)
    halo_name = (rows + peer[:, None] * slot_count + jnp.arange(slot_count, dtype=i32)).reshape(-1)
    extended_name = jnp.concatenate([jnp.arange(rows, dtype=i32), halo_name])
    turned = (jnp.arange(graphs, dtype=i32)[:, None] == peer[None, :]).astype(f32)
    halo_row = jnp.einsum("ptgk,gd->tdpk", bounds.astype(f32), turned).astype(i32)
    halo_row = halo_row.reshape(texts, graphs, graphs * slot_count)
    halo_at = jnp.repeat(jnp.arange(graphs, dtype=i32), slot_count) * rows + halo_row
    nodes = graphs * rows

    def node_stage(one_text):
        distance, listed, halo_at = one_text
        counts = jnp.sum((listed[..., None] == extended_name).astype(f32), axis=2).astype(bf16)
        table = (places == distance * rows + jnp.arange(rows, dtype=i32)[:, None]).astype(bf16)
        live = jnp.sum(table.astype(f32), axis=2).reshape(nodes, 1)

        def to_rows(by_abstract):
            return dot(table, by_abstract, ((2,), (1,)), ((0,), (0,))).reshape(nodes, -1)

        if dense:
            self_at = jnp.arange(nodes, dtype=i32).reshape(graphs, rows)
            at = jnp.concatenate([self_at, halo_at], axis=1)
            place = (at[..., None] == jnp.arange(nodes, dtype=i32)).astype(bf16)
            links = dot(counts, place, ((2,), (1,)), ((0,), (0,)))
            links = links.astype(bf16).reshape(nodes, nodes)

            def pull(values, count):
                return dot(links[:count], values, ((1,), (0,)))

            def push(values, count):
                return dot(links[:, :count], values, ((0,), (0,)))

        else:
            halo = halo_at.reshape(-1)

            def pull(values, count):
                outer = values[halo].reshape(graphs, -1, values.shape[1])
                inner = values.reshape(graphs, rows, -1)
                extended = jnp.concatenate([inner, outer], axis=1)
                out = dot(counts, extended, ((2,), (1,)), ((0,), (0,)))
                return out.reshape(nodes, -1)[:count]

            def push(values, count):
                out = dot(counts, values.reshape(graphs, rows, -1), ((1,), (1,)), ((0,), (0,)))
                inner = out[:, :rows].reshape(nodes, -1)
                return inner.at[halo].add(out[:, rows:].reshape(halo.shape[0], -1))[:count]

        up_rows = to_rows(ups)
        into_one = up_rows[:, :hidden] + push(up_rows[:, hidden:].astype(bf16), nodes) / fan
        first_rows = to_rows(firsts)
        preact_one = first_rows[:, :hidden] + pull(first_rows[:, hidden:].astype(bf16), nodes) / fan
        gelu_value, pull_back = jax.vjp(jax.nn.gelu, preact_one)
        hidden_one = (live * gelu_value).astype(bf16)
        grad_one = (live * pull_back(into_one)[0]).astype(bf16)
        aggregated = (pull(hidden_one, rows) / fan).astype(bf16)
        returned = (push(grad_one, rows) / fan).astype(bf16)
        return (
            jnp.concatenate([hidden_one[:rows], aggregated], axis=1),
            jnp.concatenate([grad_one[:rows], returned], axis=1),
            live[:rows],
        )

    normed = layer_norm(tokens, in_gain, in_bias)
    pooled_norm, pooled_context = attention(normed, doc_ids, qkv_pieces)
    out_proj = assemble(out_pieces, text, core)
    embedded = dot(pooled_context.astype(bf16), out_proj, ((1,), (1,)))
    embedded = (pooled_norm + embedded).astype(bf16)
    grads, embedded = lax.optimization_barrier((grads, embedded))
    live_grad = dot(own_table, grads.reshape(texts * rows, width), ((0,), (0,))).astype(bf16)
    up = jnp.concatenate(
        [dot(live_grad, two[0], ((1,), (1,))), dot(live_grad, two[1], ((1,), (1,)))], axis=1
    ).astype(bf16)
    ups = gather_graph(up)
    gathered = jnp.concatenate(
        [embedded] + [over_text(embedded, k) for k in range(1, texts)], axis=0
    )
    first = jnp.concatenate(
        [dot(gathered, one[0], ((1,), (0,))), dot(gathered, one[1], ((1,), (0,)))], axis=1
    ).astype(bf16)
    firsts = gather_graph(first)

    dense = texts * graphs <= 64
    per_text = (jnp.arange(texts, dtype=i32), listed.transpose(1, 0, 2, 3), halo_at)
    if dense:
        forth, back, live = jax.vmap(node_stage)(per_text)
    else:
        forth, back, live = lax.map(node_stage, per_text)
    forth = forth.reshape(texts * rows, wide)
    state_part = dot(forth[:, :hidden], two[0], ((1,), (0,))) + dot(
        forth[:, hidden:], two[1], ((1,), (0,))
    )
    back = dot(own_table, back.reshape(texts * rows, wide), ((0,), (0,))).astype(bf16)
    grad_part = dot(back[:, :hidden], one[0], ((1,), (1,))) + dot(
        back[:, hidden:], one[1], ((1,), (1,))
    )

    final = jnp.concatenate(
        [state_part.reshape(texts, rows, width), grad_part.reshape(texts, made, width)], axis=1
    )
    total = final[0]
    outgoing = final.astype(bf16)
    for k in range(1, texts):
        total = total + over_text(outgoing[k], k).astype(f32)
    node_states = (live[0] * total[:rows]).astype(bf16)
    return (node_states, total[rows:].astype(bf16))


def solution(mesh):
    rowwise = P(("text", "graph"), None)
    placed = (
        rowwise,
        rowwise,
        P(),
        P(),
        P(None, "text"),
        P(None, "text"),
        rowwise,
        P("graph", None),
        P("graph", None),
        rowwise,
        rowwise,
        rowwise,
    )

    return jax.shard_map(
        local, mesh=mesh, in_specs=placed, out_specs=(rowwise, rowwise), check_vma=False
    )
```

```python
import functools

import jax
import jax.numpy as jnp
from jax import lax
from jax.experimental import pallas as pl
from jax.experimental.pallas import tpu as pltpu
from jax.sharding import PartitionSpec as P

HEAD = 64
SEGS = 4
CORES = 2


epsilon = 1e-06
bf16 = jnp.bfloat16
f32 = jnp.float32


def dot(left, right, contract, batch=((), ())):
    return lax.dot_general(left, right, (contract, batch), preferred_element_type=f32)


def over_text(array, step):
    count = lax.axis_size("text")
    return lax.ppermute(array, "text", [(i, i ^ step) for i in range(count)])


def over_graph(array, step):
    count = lax.axis_size("graph")
    return lax.ppermute(array, "graph", [(i, i ^ step) for i in range(count)])


def over_pair(array, steps):
    texts, graphs = lax.axis_size("text"), lax.axis_size("graph")
    moves = []
    for t in range(texts):
        for g in range(graphs):
            moves.append((t * graphs + g, (t ^ steps[g % CORES]) * graphs + g))
    return lax.ppermute(array, ("text", "graph"), moves)


def natural(parts, own):
    stacked = jnp.stack(parts)
    return jnp.concatenate(
        [lax.dynamic_index_in_dim(stacked, own ^ j, 0, keepdims=True) for j in range(len(parts))]
    )


def fetch_text(shard, core):
    count = lax.axis_size("text")
    half = shard.shape[1] // CORES
    whole = [over_pair(shard, (k, k + 1)) for k in range(1, count - 1, 2)]
    split = lax.dynamic_slice_in_dim(shard, core * half, half, 1)
    return whole + [over_text(split, count - 1)]


def pieces_of(shard, fetched):
    return [shard] + [piece for got in fetched for piece in (got, over_graph(got, 1))]


def place_pieces(refs, whole, sem):
    text, core = lax.axis_index("text"), lax.axis_index("graph") % CORES
    rows, width = refs[0].shape
    count = whole.shape[0] // rows
    half = width // CORES
    spots = [(text, 0, width)]
    for k in range(1, count - 1, 2):
        spots += [(text ^ (k + core), 0, width), (text ^ (k + 1 - core), 0, width)]
    spots += [(text ^ (count - 1), core * half, half), (text ^ (count - 1), (1 - core) * half, half)]
    copies = []
    for i, (ref, (peer, lane, lanes)) in enumerate(zip(refs, spots)):
        at = pl.ds(pl.multiple_of(peer * rows, rows), rows)
        if lanes == width:
            target = whole.at[at, :]
        else:
            target = whole.at[at, pl.ds(pl.multiple_of(lane, half), half)]
        copies.append(pltpu.make_async_copy(ref, target, sem.at[i]))
    return copies


def assemble(pieces, text, core):
    parts = [pieces[0]]
    for got, swapped in zip(pieces[1:-2:2], pieces[2:-2:2]):
        parts.append(jnp.where(core == 0, got, swapped))
        parts.append(jnp.where(core == 0, swapped, got))
    got, swapped = pieces[-2:]
    parts.append(
        jnp.concatenate(
            [jnp.where(core == 0, got, swapped), jnp.where(core == 0, swapped, got)], axis=1
        )
    )
    return natural(parts, text).reshape(-1, parts[0].shape[1])


def fetch_graph(array):
    count = lax.axis_size("graph")
    return [array] + [over_graph(array, k) for k in range(CORES, count, CORES)]


def swap_cores(fetched):
    mine = jnp.stack(fetched)
    return mine, over_graph(mine, 1)


def share_cores(fetched):
    both = jnp.stack(swap_cores(fetched), axis=1)
    return both.reshape((-1,) + fetched[0].shape)


def layer_norm(tokens, in_gain, in_bias):
    states = tokens.astype(f32)
    row_mean = jnp.mean(states, axis=1, keepdims=True)
    centred = states - row_mean
    variance = jnp.mean(centred * centred, axis=1, keepdims=True)
    return (centred * lax.rsqrt(variance + epsilon) * in_gain + in_bias).astype(bf16)


def attention_kernel(*refs):
    normed_ref, doc_ref, doc_column_ref = refs[:3]
    norm_out, context_out, weights, projected, raised, sem = refs[-6:]
    copies = place_pieces(refs[3:-6], weights, sem)
    for copy in copies:
        copy.start()
    width = normed_ref.shape[1]
    blocks, length = doc_ref.shape
    pair = 2 * HEAD
    lane = lax.broadcasted_iota(jnp.int32, (2 * length, pair), 1)
    row = lax.broadcasted_iota(jnp.int32, (2 * length, pair), 0)
    own_half = (lane < HEAD) == (row < length)
    scale = jnp.where(own_half, HEAD ** (-0.5), 0.0).astype(bf16)
    ones = jnp.ones((2 * SEGS, pair), bf16)
    own_head = (lax.broadcasted_iota(jnp.int32, (4 * SEGS, 2 * length), 0) < 2 * SEGS) == (
        lax.broadcasted_iota(jnp.int32, (4 * SEGS, 2 * length), 1) < length
    )
    members = []
    lengths = []
    for b in range(blocks):
        number = lax.broadcasted_iota(jnp.int32, (2 * SEGS, length), 0)
        member = jnp.where(doc_ref[b : b + 1, :] == number, 1.0, 0.0)
        count = jnp.sum(member, axis=1, keepdims=True)[:SEGS]
        members.append(jnp.concatenate([member, member]))
        lengths.append(count)
        at = slice(b * length, (b + 1) * length)
        pooled = dot(member.astype(bf16), normed_ref[at, :], ((1,), (0,)))
        norm_out[b * SEGS : (b + 1) * SEGS, :] = pooled[:SEGS] / count
    for copy in copies:
        copy.wait()
    step = 2 * pair
    for n in range(0, 3 * width, step):
        out = dot(normed_ref[...], weights[n : n + step, :], ((1,), (1,)))
        projected[:, n : n + step] = out.astype(bf16)
    for b in range(blocks):
        at = slice(b * length, (b + 1) * length)
        same = doc_column_ref[:, b : b + 1] == doc_ref[b : b + 1, :]
        same = jnp.concatenate([same, same])
        starts = range(0, width, pair)
        for i, n in enumerate(starts):
            queries = projected[at, n : n + pair]
            keys = projected[at, width + n : width + n + pair]
            scores = dot(jnp.concatenate([queries, queries]) * scale, keys, ((1,), (1,)))
            raised[i] = jnp.where(same, jnp.exp(scores), 0.0).astype(bf16)
        totals = [dot(ones, raised[i], ((1,), (1,))) for i, n in enumerate(starts)]
        shares = []
        for i, n in enumerate(starts):
            inverse = 1.0 / totals[i]
            inverse = jnp.where(own_head, jnp.concatenate([inverse, inverse]), 0.0)
            high = inverse.astype(bf16)
            low = (inverse - high.astype(f32)).astype(bf16)
            both = dot(jnp.concatenate([high, low]), raised[i], ((1,), (0,)))
            shares.append(both[: 4 * SEGS] + both[4 * SEGS :])
        for i, n in enumerate(starts):
            values = projected[at, 2 * width + n : 2 * width + n + pair]
            mixed = dot((members[b] * shares[i]).astype(bf16), values, ((1,), (0,)))
            both = jnp.where(lane[: 2 * SEGS] < HEAD, mixed[: 2 * SEGS], mixed[2 * SEGS :])
            context_out[b * SEGS : (b + 1) * SEGS, n : n + pair] = both[:SEGS] / lengths[b]


def attention(normed, doc_ids, pieces):
    tokens, width = normed.shape
    blocks, length = doc_ids.shape
    vmem, anywhere = pl.BlockSpec(memory_space=pltpu.VMEM), pl.BlockSpec(memory_space=pl.ANY)
    pooled = jax.ShapeDtypeStruct((blocks * SEGS, width), f32)
    flops = 2 * tokens * width * 3 * width + 6 * tokens * length * width
    return pl.pallas_call(
        attention_kernel,
        out_shape=(pooled, pooled),
        in_specs=[vmem] * 3 + [anywhere] * len(pieces),
        out_specs=(vmem, vmem),
        scratch_shapes=[
            pltpu.VMEM((3 * width, width), bf16),
            pltpu.VMEM((tokens, 3 * width), bf16),
            pltpu.VMEM((width // (2 * HEAD), 2 * length, length), bf16),
            pltpu.SemaphoreType.DMA((len(pieces),)),
        ],
        cost_estimate=pl.CostEstimate(
            flops=flops, bytes_accessed=8 * width * width, transcendentals=tokens * length * width // HEAD
        ),
        name="attention",
    )(normed, doc_ids, doc_ids.T, *pieces)


def structure_kernel(mine, swapped, links, table, *, fan, slot_count, made):
    texts, nodes, _ = links.shape
    graphs = table.shape[0]
    rows = nodes // graphs
    lanes = texts * rows
    capacity = rows // texts
    text, graph = lax.axis_index("text"), lax.axis_index("graph")
    facts = [(swapped if d % CORES else mine)[d // CORES].astype(f32) for d in range(graphs)]
    tails = jnp.concatenate([each[fan : fan + 1] for each in facts]).astype(jnp.int32)
    lane = lax.broadcasted_iota(jnp.int32, (graphs, lanes), 1)

    owner_at = graphs * slot_count
    own = lane % rows - owner_at
    earlier = jnp.zeros_like(tails)
    for j in range(1, made):
        earlier += jnp.where((own >= j) & (pltpu.roll(tails, j, 1) == tails), 1, 0)
    place = (tails ^ text) * rows + (text ^ (lane // rows)) * capacity + earlier
    place = jnp.concatenate(
        [place[:, t * rows + owner_at : t * rows + owner_at + made] for t in range(texts)], axis=1
    )
    row = lax.broadcasted_iota(jnp.int32, (lanes, texts * made), 0)
    for d in range(graphs):
        table[d] = jnp.where(row == place[d : d + 1], 1.0, 0.0).astype(bf16)

    turned = tails
    bit = 1
    while bit < graphs:
        step = bit * slot_count
        up, down = pltpu.roll(turned, step, 1), pltpu.roll(turned, lanes - step, 1)
        moved = jnp.where((lane // slot_count) & bit != 0, up, down)
        turned = jnp.where(graph & bit != 0, moved, turned)
        bit *= 2
    entry = lax.broadcasted_iota(jnp.int32, (rows + owner_at, lanes), 0)
    outer = entry - rows
    name = rows + (graph ^ (outer % graphs)) * slot_count + outer // graphs
    name = jnp.where(entry < rows, entry, name).astype(f32)
    column = lax.broadcasted_iota(jnp.int32, (rows, nodes), 1)
    inner = lax.broadcasted_iota(jnp.int32, (rows, nodes), 0)
    base = lax.broadcasted_iota(jnp.int32, (graphs, nodes), 0) * rows
    for d in range(graphs):
        counts = jnp.zeros((rows + owner_at, lanes), f32)
        for f in range(fan):
            counts += jnp.where(facts[d][f : f + 1] == name, 1.0, 0.0)
        counts = counts.T.astype(bf16)
        for t in range(texts):
            spots = [jnp.where(column == inner + d * rows, 1.0, 0.0)]
            for k in range(slot_count):
                at = t * rows + d * slot_count + k
                target = base + turned[:, at : at + 1]
                spots.append(jnp.where(column[:graphs] == target, 1.0, 0.0))
            spots = jnp.concatenate(spots).astype(bf16)
            linked = dot(counts[t * rows : (t + 1) * rows], spots, ((1,), (0,)))
            links[t, d * rows : (d + 1) * rows, :] = linked.astype(bf16)


def node_kernel(mine, swapped, up_mine, up_swapped, table, links, one, two, out, own, live_out, *refs, fan):
    first_self, first_next, up_self, up_next, live, kept = refs
    texts, nodes, _ = links.shape
    graphs = table.shape[0]
    rows = nodes // graphs
    made = table.shape[2] // texts
    hidden = two.shape[1]
    ones = jnp.ones((texts * made, live.shape[2]), bf16)
    for d in range(graphs):
        chosen = table[d]
        values = (swapped if d % CORES else mine)[d // CORES]
        ups = (up_swapped if d % CORES else up_mine)[d // CORES]
        for target, value in (
            (live, ones),
            (first_self, values[:, :hidden]),
            (first_next, values[:, hidden:]),
            (up_self, ups[:, :hidden]),
            (up_next, ups[:, hidden:]),
        ):
            placed = dot(chosen, value, ((1,), (0,))).astype(bf16)
            for t in range(texts):
                target[t, d * rows : (d + 1) * rows, :] = placed[t * rows : (t + 1) * rows]
    for t in range(texts):
        linked = links[t]
        x = first_self[t].astype(f32) + dot(linked, first_next[t], ((1,), (0,))) / fan
        into = up_self[t].astype(f32) + dot(linked, up_next[t], ((0,), (0,))) / fan
        alive = live[t][:, :1].astype(f32)
        square = x * x
        slope = 0.7978845608028654 * (1.0 + 3.0 * 0.044715 * square)
        half = 0.5 * (1.0 + jnp.tanh(0.7978845608028654 * (x + 0.044715 * square * x)))
        value = (alive * (x * half)).astype(bf16)
        grad = (alive * ((half + 2.0 * x * half * (1.0 - half) * slope) * into)).astype(bf16)
        at = slice(t * rows, (t + 1) * rows)
        kept[0, at, :] = value[:rows]
        kept[1, at, :] = (dot(linked[:rows], value, ((1,), (0,))) / fan).astype(bf16)
        kept[2, at, :] = grad[:rows]
        kept[3, at, :] = (dot(linked[:, :rows], grad, ((0,), (0,))) / fan).astype(bf16)
    state = dot(kept[0], two[0], ((1,), (0,))) + dot(kept[1], two[1], ((1,), (0,)))
    back = [dot(table[0], kept[i], ((0,), (0,))).astype(bf16) for i in (2, 3)]
    returned = dot(back[0], one[0], ((1,), (1,))) + dot(back[1], one[1], ((1,), (1,)))
    for t in range(texts):
        out[t, :rows, :] = state[t * rows : (t + 1) * rows].astype(bf16)
        out[t, rows:, :] = returned[t * made : (t + 1) * made].astype(bf16)
    own[:rows, :] = state[:rows]
    own[rows:, :] = returned[:made]
    live_out[...] = live[0, :rows, :].astype(f32)


def unpack_kernel(mine, swapped, one, two, *, depth, share):
    graph = lax.axis_index("graph")
    graphs = CORES * mine.shape[0]
    hidden, width = two.shape[1:]
    lanes = mine.shape[2]
    same = graph % CORES == 0
    for g in range(graphs):
        z = (graph // CORES) ^ (g // CORES)
        near, far = mine[z], swapped[z]
        got = jnp.where(same == (g % CORES == 0), near, far)
        half, j = g // (graphs // 2), g % (graphs // 2)
        one[half, j * depth : (j + 1) * depth, :] = got[:depth, :hidden]
        for m in range(width // lanes):
            part = got[depth + m * share : depth + (m + 1) * share]
            two[half, j * share : (j + 1) * share, m * lanes : (m + 1) * lanes] = part


def unpack(mine, swapped, depth, share, hidden, width):
    vmem = pl.BlockSpec(memory_space=pltpu.VMEM)
    return pl.pallas_call(
        functools.partial(unpack_kernel, depth=depth, share=share),
        out_shape=(
            jax.ShapeDtypeStruct((2, width, hidden), bf16),
            jax.ShapeDtypeStruct((2, hidden, width), bf16),
        ),
        in_specs=[vmem] * 2,
        out_specs=(vmem, vmem),
        cost_estimate=pl.CostEstimate(flops=10**8, bytes_accessed=10**6, transcendentals=0),
        name="unpack",
    )(mine, swapped)


def structure(mine, swapped, texts, graphs, rows, **sizes):
    vmem = pl.BlockSpec(memory_space=pltpu.VMEM)
    nodes, made = graphs * rows, sizes["made"]
    return pl.pallas_call(
        functools.partial(structure_kernel, **sizes),
        out_shape=(
            jax.ShapeDtypeStruct((texts, nodes, nodes), bf16),
            jax.ShapeDtypeStruct((graphs, texts * rows, texts * made), bf16),
        ),
        in_specs=[vmem] * 2,
        out_specs=(vmem, vmem),
        cost_estimate=pl.CostEstimate(flops=10**9, bytes_accessed=10**6, transcendentals=0),
        name="structure",
    )(mine, swapped)


def node_stage_parts(arrays, fan):
    vmem = pl.BlockSpec(memory_space=pltpu.VMEM)
    table, links, _, two = arrays[4:]
    texts, nodes, _ = links.shape
    rows = nodes // table.shape[0]
    made = table.shape[2] // texts
    hidden, width = two.shape[1:]
    return pl.pallas_call(
        functools.partial(node_kernel, fan=fan),
        out_shape=(
            jax.ShapeDtypeStruct((texts, rows + made, width), bf16),
            jax.ShapeDtypeStruct((rows + made, width), f32),
            jax.ShapeDtypeStruct((rows, 128), f32),
        ),
        in_specs=[vmem] * len(arrays),
        out_specs=(vmem,) * 3,
        scratch_shapes=[pltpu.VMEM((texts, nodes, hidden), bf16)] * 4
        + [pltpu.VMEM((texts, nodes, 128), bf16), pltpu.VMEM((4, texts * rows, hidden), bf16)],
        cost_estimate=pl.CostEstimate(flops=10**9, bytes_accessed=10**6, transcendentals=10**6),
        name="nodes",
    )(*arrays)


def local(
    tokens,
    doc_ids,
    in_gain,
    in_bias,
    attn_qkv,
    attn_out,
    owner_text,
    sage_one,
    sage_two,
    neighbours,
    boundary,
    out_grad,
):
    width = tokens.shape[1]
    texts, graphs = lax.axis_size("text"), lax.axis_size("graph")
    text, graph = lax.axis_index("text"), lax.axis_index("graph")
    core = graph % CORES
    rows = out_grad.shape[0]
    made = owner_text.shape[0]
    capacity = rows // texts
    fan = neighbours.shape[1]
    slot_count = boundary.shape[1]
    i32 = jnp.int32

    qkv_shard, out_shard = attn_qkv.T, attn_out.T
    qkv_fetched = fetch_text(qkv_shard, core)
    out_fetched = fetch_text(out_shard, core)
    qkv_pieces = pieces_of(qkv_shard, qkv_fetched)

    depth = sage_one.shape[0]
    share = depth // texts
    hidden = (graphs // 2) * share
    lanes = next(n for n in range(128, width + 1, 128) if n >= hidden and width % n == 0)
    column = jnp.arange(lanes, dtype=i32)
    wanted = (column // share) * depth + text * share + column % share
    wanted = jnp.where(column < hidden, wanted, -1)
    chosen = (jnp.arange(width, dtype=i32)[:, None] == wanted[None, :]).astype(bf16)
    one_share = dot(sage_one, chosen, ((1,), (0,))).astype(bf16)
    two_share = lax.dynamic_slice_in_dim(sage_two, text * share, share, 0)
    packed = jnp.concatenate(
        [one_share] + [two_share[:, i : i + lanes] for i in range(0, width, lanes)], axis=0
    )
    sage_fetched = fetch_graph(packed)

    tail = jnp.concatenate([boundary.reshape(-1), owner_text.reshape(-1)])
    tail_count = tail.shape[0]
    tail = jnp.pad(tail, (0, -tail_count % rows)).reshape(-1, rows)
    facts = jnp.concatenate([neighbours.T, tail], axis=0).astype(bf16)
    fact_rows = facts.shape[0]
    facts = jnp.pad(facts, ((0, rows - fact_rows), (0, -rows % 128)))
    outset = jnp.concatenate([out_grad, facts], axis=1)
    outset = [outset] + [over_text(outset, k) for k in range(1, texts)]
    grads = jnp.concatenate([part[:, :width] for part in outset], axis=0)
    facts = jnp.concatenate([part[:fact_rows, width : width + rows] for part in outset], axis=1)

    def tail_of(facts):
        tail = facts[..., fan:, :].reshape(facts.shape[:-2] + (fact_rows - fan, texts, rows))
        tail = jnp.moveaxis(tail, -2, -3).reshape(facts.shape[:-2] + (texts, -1))
        return tail.astype(i32)

    def slot_places(owners):
        same = owners[..., :, None] == owners[..., None, :]
        order = jnp.arange(made, dtype=i32)
        earlier = jnp.sum((same & (order[None, :] < order[:, None])).astype(i32), axis=-1)
        source = text ^ jnp.arange(texts, dtype=i32)
        place = (owners ^ text) * rows + source[:, None] * capacity + earlier
        return place.reshape(owners.shape[:-2] + (1, texts * made))

    own_places = slot_places(tail_of(facts)[:, tail_count - made : tail_count])
    own_table = (own_places == jnp.arange(texts * rows, dtype=i32)[:, None]).astype(bf16)
    wide = 2 * hidden
    facts_fetched = fetch_graph(facts)

    one, two = unpack(*swap_cores(sage_fetched), depth, share, hidden, width)
    normed = layer_norm(tokens, in_gain, in_bias)
    pooled_norm, pooled_context = attention(normed, doc_ids, qkv_pieces)
    out_fetched, facts_fetched, pooled_context = lax.optimization_barrier(
        (out_fetched, facts_fetched, pooled_context)
    )
    out_pieces = pieces_of(out_shard, out_fetched)
    out_proj = assemble(out_pieces, text, core)
    embedded = dot(pooled_context.astype(bf16), out_proj, ((1,), (1,)))
    embedded = (pooled_norm + embedded).astype(bf16)
    grads, embedded = lax.optimization_barrier((grads, embedded))
    live_grad = dot(own_table, grads, ((0,), (0,))).astype(bf16)
    up = jnp.concatenate(
        [dot(live_grad, two[0], ((1,), (1,))), dot(live_grad, two[1], ((1,), (1,)))], axis=1
    ).astype(bf16)
    up_fetched = fetch_graph(up)
    gathered = jnp.concatenate(
        [embedded] + [over_text(embedded, k) for k in range(1, texts)], axis=0
    )
    first = jnp.concatenate(
        [dot(gathered, one[0], ((1,), (0,))), dot(gathered, one[1], ((1,), (0,)))], axis=1
    ).astype(bf16)
    first_fetched = fetch_graph(first)

    if texts * rows == 128 and tail_count == rows and capacity * texts == rows:
        links, table = structure(
            *swap_cores(facts_fetched),
            texts,
            graphs,
            rows,
            fan=fan,
            slot_count=slot_count,
            made=made,
        )
        parts = (*swap_cores(first_fetched), *swap_cores(up_fetched))
        outgoing, total, live = node_stage_parts((*parts, table, links, one, two), fan)
        live = live[:, :1]
    else:
        facts = share_cores(facts_fetched)
        ups = share_cores(up_fetched)
        firsts = share_cores(first_fetched)
        listed = facts[:, :fan].reshape(graphs, fan, texts, rows).transpose(0, 2, 3, 1).astype(i32)
        tail = tail_of(facts)
        bounds = tail[..., : tail_count - made].reshape(graphs, texts, graphs, slot_count)
        owners = tail[..., tail_count - made : tail_count]
        places = slot_places(owners)
        peer = graph ^ jnp.arange(graphs, dtype=i32)
        halo_name = (rows + peer[:, None] * slot_count + jnp.arange(slot_count, dtype=i32)).reshape(-1)
        extended_name = jnp.concatenate([jnp.arange(rows, dtype=i32), halo_name])
        turned = (jnp.arange(graphs, dtype=i32)[:, None] == peer[None, :]).astype(f32)
        halo_row = jnp.einsum("ptgk,gd->tdpk", bounds.astype(f32), turned).astype(i32)
        halo_row = halo_row.reshape(texts, graphs, graphs * slot_count)
        halo_at = jnp.repeat(jnp.arange(graphs, dtype=i32), slot_count) * rows + halo_row
        nodes = graphs * rows

        def node_stage(one_text):
            distance, listed, halo_at = one_text
            counts = jnp.sum((listed[..., None] == extended_name).astype(f32), axis=2).astype(bf16)
            table = (places == distance * rows + jnp.arange(rows, dtype=i32)[:, None]).astype(bf16)
            live = jnp.sum(table.astype(f32), axis=2).reshape(nodes, 1)

            def to_rows(by_abstract):
                return dot(table, by_abstract, ((2,), (1,)), ((0,), (0,))).reshape(nodes, -1)

            halo = halo_at.reshape(-1)

            def pull(values, count):
                outer = values[halo].reshape(graphs, -1, values.shape[1])
                inner = values.reshape(graphs, rows, -1)
                extended = jnp.concatenate([inner, outer], axis=1)
                out = dot(counts, extended, ((2,), (1,)), ((0,), (0,)))
                return out.reshape(nodes, -1)[:count]

            def push(values, count):
                out = dot(counts, values.reshape(graphs, rows, -1), ((1,), (1,)), ((0,), (0,)))
                inner = out[:, :rows].reshape(nodes, -1)
                return inner.at[halo].add(out[:, rows:].reshape(halo.shape[0], -1))[:count]

            up_rows = to_rows(ups)
            into_one = up_rows[:, :hidden] + push(up_rows[:, hidden:].astype(bf16), nodes) / fan
            first_rows = to_rows(firsts)
            preact_one = first_rows[:, :hidden] + pull(first_rows[:, hidden:].astype(bf16), nodes) / fan
            gelu_value, pull_back = jax.vjp(jax.nn.gelu, preact_one)
            hidden_one = (live * gelu_value).astype(bf16)
            grad_one = (live * pull_back(into_one)[0]).astype(bf16)
            aggregated = (pull(hidden_one, rows) / fan).astype(bf16)
            returned = (push(grad_one, rows) / fan).astype(bf16)
            return (
                jnp.concatenate([hidden_one[:rows], aggregated], axis=1),
                jnp.concatenate([grad_one[:rows], returned], axis=1),
                live[:rows],
            )

        per_text = (jnp.arange(texts, dtype=i32), listed.transpose(1, 0, 2, 3), halo_at)
        forth, back, live = lax.map(node_stage, per_text)
        forth = forth.reshape(texts * rows, wide)
        state_part = dot(forth[:, :hidden], two[0], ((1,), (0,))) + dot(
            forth[:, hidden:], two[1], ((1,), (0,))
        )
        back = dot(own_table, back.reshape(texts * rows, wide), ((0,), (0,))).astype(bf16)
        grad_part = dot(back[:, :hidden], one[0], ((1,), (1,))) + dot(
            back[:, hidden:], one[1], ((1,), (1,))
        )

        final = jnp.concatenate(
            [state_part.reshape(texts, rows, width), grad_part.reshape(texts, made, width)], axis=1
        )
        total, outgoing, live = final[0], final.astype(bf16), live[0]
    for k in range(1, texts):
        total = total + over_text(outgoing[k], k).astype(f32)
    node_states = (live * total[:rows]).astype(bf16)
    return (node_states, total[rows:].astype(bf16))


def solution(mesh):
    rowwise = P(("text", "graph"), None)
    placed = (
        rowwise,
        rowwise,
        P(),
        P(),
        P(None, "text"),
        P(None, "text"),
        rowwise,
        P("graph", None),
        P("graph", None),
        rowwise,
        rowwise,
        rowwise,
    )

    return jax.shard_map(
        local, mesh=mesh, in_specs=placed, out_specs=(rowwise, rowwise), check_vma=False
    )
```

```python
import functools

import jax
import jax.numpy as jnp
from jax import lax
from jax.experimental import pallas as pl
from jax.experimental.pallas import tpu as pltpu
from jax.sharding import PartitionSpec as P

HEAD = 64
SEGS = 4
CORES = 2


epsilon = 1e-06
bf16 = jnp.bfloat16
f32 = jnp.float32


def dot(left, right, contract, batch=((), ())):
    return lax.dot_general(left, right, (contract, batch), preferred_element_type=f32)


def over_text(array, step):
    count = lax.axis_size("text")
    return lax.ppermute(array, "text", [(i, i ^ step) for i in range(count)])


def over_graph(array, step):
    count = lax.axis_size("graph")
    return lax.ppermute(array, "graph", [(i, i ^ step) for i in range(count)])


def over_pair(array, steps):
    texts, graphs = lax.axis_size("text"), lax.axis_size("graph")
    moves = []
    for t in range(texts):
        for g in range(graphs):
            moves.append((t * graphs + g, (t ^ steps[g % CORES]) * graphs + g))
    return lax.ppermute(array, ("text", "graph"), moves)


def natural(parts, own):
    stacked = jnp.stack(parts)
    return jnp.concatenate(
        [lax.dynamic_index_in_dim(stacked, own ^ j, 0, keepdims=True) for j in range(len(parts))]
    )


def fetch_text(shard, core):
    count = lax.axis_size("text")
    half = shard.shape[1] // CORES
    whole = [over_pair(shard, (k, k + 1)) for k in range(1, count - 1, 2)]
    split = lax.dynamic_slice_in_dim(shard, core * half, half, 1)
    return whole + [over_text(split, count - 1)]


def pieces_of(shard, fetched):
    swapped = [over_graph(got, 1) for got in fetched]
    return [shard] + [piece for both in zip(fetched, swapped) for piece in both]


def place_pieces(refs, whole, sem):
    text, core = lax.axis_index("text"), lax.axis_index("graph") % CORES
    rows, width = refs[0].shape
    count = whole.shape[0] // rows
    half = width // CORES
    spots = [(text, 0, width)]
    for k in range(1, count - 1, 2):
        spots += [(text ^ (k + core), 0, width), (text ^ (k + 1 - core), 0, width)]
    spots += [(text ^ (count - 1), core * half, half), (text ^ (count - 1), (1 - core) * half, half)]
    copies = []
    for i, (ref, (peer, lane, lanes)) in enumerate(zip(refs, spots)):
        at = pl.ds(pl.multiple_of(peer * rows, rows), rows)
        if lanes == width:
            target = whole.at[at, :]
        else:
            target = whole.at[at, pl.ds(pl.multiple_of(lane, half), half)]
        copies.append(pltpu.make_async_copy(ref, target, sem.at[i]))
    return copies


def assemble(pieces, text, core):
    parts = [pieces[0]]
    for got, swapped in zip(pieces[1:-2:2], pieces[2:-2:2]):
        parts.append(jnp.where(core == 0, got, swapped))
        parts.append(jnp.where(core == 0, swapped, got))
    got, swapped = pieces[-2:]
    parts.append(
        jnp.concatenate(
            [jnp.where(core == 0, got, swapped), jnp.where(core == 0, swapped, got)], axis=1
        )
    )
    return natural(parts, text).reshape(-1, parts[0].shape[1])


def fetch_graph(array):
    count = lax.axis_size("graph")
    return [array] + [over_graph(array, k) for k in range(CORES, count, CORES)]


def swap_cores(fetched):
    mine = jnp.stack(fetched)
    return mine, over_graph(mine, 1)


def share_cores(fetched):
    both = jnp.stack(swap_cores(fetched), axis=1)
    return both.reshape((-1,) + fetched[0].shape)


def layer_norm(tokens, in_gain, in_bias):
    states = tokens.astype(f32)
    row_mean = jnp.mean(states, axis=1, keepdims=True)
    centred = states - row_mean
    variance = jnp.mean(centred * centred, axis=1, keepdims=True)
    return (centred * lax.rsqrt(variance + epsilon) * in_gain + in_bias).astype(bf16)


def place_shares(mine, swapped, one, two, sem, depth):
    graph = lax.axis_index("graph")
    count, height, lanes = mine.shape
    width = two.shape[2]
    share = (height - depth) * lanes // width
    per_half = CORES * count // 2
    copies = []
    for k in range(count):
        for source, core in ((mine, graph % CORES), (swapped, 1 - graph % CORES)):
            peer = ((graph // CORES) ^ k) * CORES + core
            half, j = peer // per_half, peer % per_half
            at = pl.ds(pl.multiple_of(j * depth, depth), depth)
            moves = [(source.at[k, :depth, :], one.at[half, at, :])]
            at = pl.ds(pl.multiple_of(j * share, share), share)
            for m in range(width // lanes):
                start = depth + m * share
                part = source.at[k, start : start + share, :]
                moves.append((part, two.at[half, at, m * lanes : (m + 1) * lanes]))
            for source_at, target in moves:
                copies.append(pltpu.make_async_copy(source_at, target, sem.at[len(copies)]))
    return copies


def attention_kernel(*refs, pieces, depth):
    normed_ref, doc_ref, doc_column_ref = refs[:3]
    weights, projected, raised, sem, share_sem = refs[-5:]
    copies = place_pieces(refs[3 : 3 + pieces], weights, sem)
    outputs = refs[3 + pieces : -5]
    moves = []
    if depth:
        moves = place_shares(*outputs[:2], *outputs[-2:], share_sem, depth)
        outputs = outputs[2:]
    norm_out, context_out = outputs[:2]
    for copy in copies:
        copy.start()
    for copy in moves:
        copy.start()
    width = normed_ref.shape[1]
    blocks, length = doc_ref.shape
    pair = 2 * HEAD
    lane = lax.broadcasted_iota(jnp.int32, (2 * length, pair), 1)
    row = lax.broadcasted_iota(jnp.int32, (2 * length, pair), 0)
    own_half = (lane < HEAD) == (row < length)
    scale = jnp.where(own_half, HEAD ** (-0.5), 0.0).astype(bf16)
    ones = jnp.ones((2 * SEGS, pair), bf16)
    own_head = (lax.broadcasted_iota(jnp.int32, (4 * SEGS, 2 * length), 0) < 2 * SEGS) == (
        lax.broadcasted_iota(jnp.int32, (4 * SEGS, 2 * length), 1) < length
    )
    members = []
    lengths = []
    for b in range(blocks):
        number = lax.broadcasted_iota(jnp.int32, (2 * SEGS, length), 0)
        member = jnp.where(doc_ref[b : b + 1, :] == number, 1.0, 0.0)
        count = jnp.sum(member, axis=1, keepdims=True)[:SEGS]
        members.append(jnp.concatenate([member, member]))
        lengths.append(count)
        at = slice(b * length, (b + 1) * length)
        pooled = dot(member.astype(bf16), normed_ref[at, :], ((1,), (0,)))
        norm_out[b * SEGS : (b + 1) * SEGS, :] = pooled[:SEGS] / count
    for copy in copies:
        copy.wait()
    step = 2 * pair
    for n in range(0, 3 * width, step):
        out = dot(normed_ref[...], weights[n : n + step, :], ((1,), (1,)))
        projected[:, n : n + step] = out.astype(bf16)
    for b in range(blocks):
        at = slice(b * length, (b + 1) * length)
        same = doc_column_ref[:, b : b + 1] == doc_ref[b : b + 1, :]
        same = jnp.concatenate([same, same])
        starts = range(0, width, pair)
        for i, n in enumerate(starts):
            queries = projected[at, n : n + pair]
            keys = projected[at, width + n : width + n + pair]
            scores = dot(jnp.concatenate([queries, queries]) * scale, keys, ((1,), (1,)))
            raised[i] = jnp.where(same, jnp.exp(scores), 0.0).astype(bf16)
        totals = [dot(ones, raised[i], ((1,), (1,))) for i, n in enumerate(starts)]
        shares = []
        for i, n in enumerate(starts):
            inverse = 1.0 / totals[i]
            inverse = jnp.where(own_head, jnp.concatenate([inverse, inverse]), 0.0)
            high = inverse.astype(bf16)
            low = (inverse - high.astype(f32)).astype(bf16)
            both = dot(jnp.concatenate([high, low]), raised[i], ((1,), (0,)))
            shares.append(both[: 4 * SEGS] + both[4 * SEGS :])
        for i, n in enumerate(starts):
            values = projected[at, 2 * width + n : 2 * width + n + pair]
            mixed = dot((members[b] * shares[i]).astype(bf16), values, ((1,), (0,)))
            both = jnp.where(lane[: 2 * SEGS] < HEAD, mixed[: 2 * SEGS], mixed[2 * SEGS :])
            context_out[b * SEGS : (b + 1) * SEGS, n : n + pair] = both[:SEGS] / lengths[b]
    for copy in moves:
        copy.wait()


def attention(normed, doc_ids, pieces, shares, depth, hidden):
    tokens, width = normed.shape
    blocks, length = doc_ids.shape
    vmem, anywhere = pl.BlockSpec(memory_space=pltpu.VMEM), pl.BlockSpec(memory_space=pl.ANY)
    pooled = jax.ShapeDtypeStruct((blocks * SEGS, width), f32)
    placed, moves = (), 1
    if shares:
        count, _, lanes = shares[0].shape
        placed = (
            jax.ShapeDtypeStruct((2, width, lanes), bf16),
            jax.ShapeDtypeStruct((2, hidden, width), bf16),
        )
        moves = CORES * count * (1 + width // lanes)
    flops = 2 * tokens * width * 3 * width + 6 * tokens * length * width
    return pl.pallas_call(
        functools.partial(attention_kernel, pieces=len(pieces), depth=depth if shares else 0),
        out_shape=(pooled, pooled) + placed,
        in_specs=[vmem] * 3 + [anywhere] * (len(pieces) + len(shares)),
        out_specs=(vmem,) * (2 + len(placed)),
        scratch_shapes=[
            pltpu.VMEM((3 * width, width), bf16),
            pltpu.VMEM((tokens, 3 * width), bf16),
            pltpu.VMEM((width // (2 * HEAD), 2 * length, length), bf16),
            pltpu.SemaphoreType.DMA((len(pieces),)),
            pltpu.SemaphoreType.DMA((moves,)),
        ],
        cost_estimate=pl.CostEstimate(
            flops=flops, bytes_accessed=8 * width * width, transcendentals=tokens * length * width // HEAD
        ),
        name="attention",
    )(normed, doc_ids, doc_ids.T, *pieces, *shares)


def structure_kernel(mine, swapped, links, table, *, fan, slot_count, made):
    texts, nodes, _ = links.shape
    graphs = table.shape[0]
    rows = nodes // graphs
    lanes = texts * rows
    capacity = rows // texts
    text, graph = lax.axis_index("text"), lax.axis_index("graph")
    skip = texts * made
    facts = [
        (swapped if d % CORES else mine)[d // CORES, skip:, :lanes].astype(f32)
        for d in range(graphs)
    ]
    tails = jnp.concatenate([each[fan : fan + 1] for each in facts]).astype(jnp.int32)
    lane = lax.broadcasted_iota(jnp.int32, (graphs, lanes), 1)

    owner_at = graphs * slot_count
    own = lane % rows - owner_at
    earlier = jnp.zeros_like(tails)
    for j in range(1, made):
        earlier += jnp.where((own >= j) & (pltpu.roll(tails, j, 1) == tails), 1, 0)
    place = (tails ^ text) * rows + (text ^ (lane // rows)) * capacity + earlier
    place = jnp.concatenate(
        [place[:, t * rows + owner_at : t * rows + owner_at + made] for t in range(texts)], axis=1
    )
    row = lax.broadcasted_iota(jnp.int32, (lanes, texts * made), 0)
    for d in range(graphs):
        table[d] = jnp.where(row == place[d : d + 1], 1.0, 0.0).astype(bf16)

    turned = tails
    bit = 1
    while bit < graphs:
        step = bit * slot_count
        up, down = pltpu.roll(turned, step, 1), pltpu.roll(turned, lanes - step, 1)
        moved = jnp.where((lane // slot_count) & bit != 0, up, down)
        turned = jnp.where(graph & bit != 0, moved, turned)
        bit *= 2
    entry = lax.broadcasted_iota(jnp.int32, (rows + owner_at, lanes), 0)
    outer = entry - rows
    name = rows + (graph ^ (outer % graphs)) * slot_count + outer // graphs
    name = jnp.where(entry < rows, entry, name).astype(f32)
    column = lax.broadcasted_iota(jnp.int32, (rows, nodes), 1)
    inner = lax.broadcasted_iota(jnp.int32, (rows, nodes), 0)
    base = lax.broadcasted_iota(jnp.int32, (graphs, nodes), 0) * rows
    for d in range(graphs):
        counts = jnp.zeros((rows + owner_at, lanes), f32)
        for f in range(fan):
            counts += jnp.where(facts[d][f : f + 1] == name, 1.0, 0.0)
        counts = counts.T.astype(bf16)
        for t in range(texts):
            spots = [jnp.where(column == inner + d * rows, 1.0, 0.0)]
            for k in range(slot_count):
                at = t * rows + d * slot_count + k
                target = base + turned[:, at : at + 1]
                spots.append(jnp.where(column[:graphs] == target, 1.0, 0.0))
            spots = jnp.concatenate(spots).astype(bf16)
            linked = dot(counts[t * rows : (t + 1) * rows], spots, ((1,), (0,)))
            links[t, d * rows : (d + 1) * rows, :] = linked.astype(bf16)


def node_kernel(mine, swapped, up_mine, up_swapped, table, links, one, two, *refs, fan):
    first_self, first_next, up_self, up_next, live, kept = refs[-6:]
    own, live_out = refs[-8:-6]
    texts, nodes, _ = links.shape
    graphs = table.shape[0]
    rows = nodes // graphs
    made = table.shape[2] // texts
    hidden = two.shape[1]
    ones = jnp.ones((texts * made, live.shape[2]), bf16)
    for d in range(graphs):
        chosen = table[d]
        values = (swapped if d % CORES else mine)[d // CORES]
        ups = (up_swapped if d % CORES else up_mine)[d // CORES, : texts * made]
        for target, value in (
            (live, ones),
            (first_self, values[:, :hidden]),
            (first_next, values[:, hidden:]),
            (up_self, ups[:, :hidden]),
            (up_next, ups[:, hidden:]),
        ):
            placed = dot(chosen, value, ((1,), (0,))).astype(bf16)
            for t in range(texts):
                target[t, d * rows : (d + 1) * rows, :] = placed[t * rows : (t + 1) * rows]
    for t in range(texts):
        linked = links[t]
        x = first_self[t].astype(f32) + dot(linked, first_next[t], ((1,), (0,))) / fan
        into = up_self[t].astype(f32) + dot(linked, up_next[t], ((0,), (0,))) / fan
        alive = live[t][:, :1].astype(f32)
        square = x * x
        slope = 0.7978845608028654 * (1.0 + 3.0 * 0.044715 * square)
        half = 0.5 * (1.0 + jnp.tanh(0.7978845608028654 * (x + 0.044715 * square * x)))
        value = (alive * (x * half)).astype(bf16)
        grad = (alive * ((half + 2.0 * x * half * (1.0 - half) * slope) * into)).astype(bf16)
        at = slice(t * rows, (t + 1) * rows)
        kept[0, at, :] = value[:rows]
        kept[1, at, :] = (dot(linked[:rows], value, ((1,), (0,))) / fan).astype(bf16)
        kept[2, at, :] = grad[:rows]
        kept[3, at, :] = (dot(linked[:, :rows], grad, ((0,), (0,))) / fan).astype(bf16)
    state = dot(kept[0], two[0], ((1,), (0,))) + dot(kept[1], two[1], ((1,), (0,)))
    back = [dot(table[0], kept[i], ((0,), (0,))).astype(bf16) for i in (2, 3)]
    returned = dot(back[0], one[0, :, :hidden], ((1,), (1,))) + dot(
        back[1], one[1, :, :hidden], ((1,), (1,))
    )
    for t in range(1, texts):
        refs[t - 1][:rows, :] = state[t * rows : (t + 1) * rows].astype(bf16)
        refs[t - 1][rows:, :] = returned[t * made : (t + 1) * made].astype(bf16)
    own[:rows, :] = state[:rows]
    own[rows:, :] = returned[:made]
    live_out[...] = live[0, :rows, :].astype(f32)


def unpack_kernel(mine, swapped, one, two, *, depth, share):
    graph = lax.axis_index("graph")
    graphs = CORES * mine.shape[0]
    width = two.shape[2]
    lanes = mine.shape[2]
    same = graph % CORES == 0
    for g in range(graphs):
        z = (graph // CORES) ^ (g // CORES)
        near, far = mine[z], swapped[z]
        got = jnp.where(same == (g % CORES == 0), near, far)
        half, j = g // (graphs // 2), g % (graphs // 2)
        one[half, j * depth : (j + 1) * depth, :] = got[:depth]
        for m in range(width // lanes):
            part = got[depth + m * share : depth + (m + 1) * share]
            two[half, j * share : (j + 1) * share, m * lanes : (m + 1) * lanes] = part


def unpack(mine, swapped, depth, share, hidden, width):
    vmem = pl.BlockSpec(memory_space=pltpu.VMEM)
    return pl.pallas_call(
        functools.partial(unpack_kernel, depth=depth, share=share),
        out_shape=(
            jax.ShapeDtypeStruct((2, width, mine.shape[2]), bf16),
            jax.ShapeDtypeStruct((2, hidden, width), bf16),
        ),
        in_specs=[vmem] * 2,
        out_specs=(vmem, vmem),
        cost_estimate=pl.CostEstimate(flops=10**8, bytes_accessed=10**6, transcendentals=0),
        name="unpack",
    )(mine, swapped)


def structure(mine, swapped, texts, graphs, rows, **sizes):
    vmem = pl.BlockSpec(memory_space=pltpu.VMEM)
    nodes, made = graphs * rows, sizes["made"]
    return pl.pallas_call(
        functools.partial(structure_kernel, **sizes),
        out_shape=(
            jax.ShapeDtypeStruct((texts, nodes, nodes), bf16),
            jax.ShapeDtypeStruct((graphs, texts * rows, texts * made), bf16),
        ),
        in_specs=[vmem] * 2,
        out_specs=(vmem, vmem),
        cost_estimate=pl.CostEstimate(flops=10**9, bytes_accessed=10**6, transcendentals=0),
        name="structure",
    )(mine, swapped)


def node_stage_parts(arrays, fan):
    vmem = pl.BlockSpec(memory_space=pltpu.VMEM)
    table, links, _, two = arrays[4:]
    texts, nodes, _ = links.shape
    rows = nodes // table.shape[0]
    made = table.shape[2] // texts
    hidden, width = two.shape[1:]
    return pl.pallas_call(
        functools.partial(node_kernel, fan=fan),
        out_shape=[jax.ShapeDtypeStruct((rows + made, width), bf16)] * (texts - 1)
        + [
            jax.ShapeDtypeStruct((rows + made, width), f32),
            jax.ShapeDtypeStruct((rows, 128), f32),
        ],
        in_specs=[vmem] * len(arrays),
        out_specs=[vmem] * (texts + 1),
        scratch_shapes=[pltpu.VMEM((texts, nodes, hidden), bf16)] * 4
        + [pltpu.VMEM((texts, nodes, 128), bf16), pltpu.VMEM((4, texts * rows, hidden), bf16)],
        cost_estimate=pl.CostEstimate(flops=10**9, bytes_accessed=10**6, transcendentals=10**6),
        name="nodes",
    )(*arrays)


def combine_kernel(own, live, *refs):
    states, grads = refs[-2:]
    rows = states.shape[0]
    total = own[...]
    for part in refs[:-2]:
        total += part[...].astype(f32)
    states[...] = (live[:, :1] * total[:rows]).astype(bf16)
    grads[...] = total[rows:].astype(bf16)


def combine(own, live, got):
    vmem = pl.BlockSpec(memory_space=pltpu.VMEM)
    rows, width = live.shape[0], own.shape[1]
    return pl.pallas_call(
        combine_kernel,
        out_shape=(
            jax.ShapeDtypeStruct((rows, width), bf16),
            jax.ShapeDtypeStruct((own.shape[0] - rows, width), bf16),
        ),
        in_specs=[vmem] * (2 + len(got)),
        out_specs=(vmem, vmem),
        name="combine",
    )(own, live, *got)


def local(
    tokens,
    doc_ids,
    in_gain,
    in_bias,
    attn_qkv,
    attn_out,
    owner_text,
    sage_one,
    sage_two,
    neighbours,
    boundary,
    out_grad,
):
    width = tokens.shape[1]
    texts, graphs = lax.axis_size("text"), lax.axis_size("graph")
    text, graph = lax.axis_index("text"), lax.axis_index("graph")
    core = graph % CORES
    rows = out_grad.shape[0]
    made = owner_text.shape[0]
    capacity = rows // texts
    fan = neighbours.shape[1]
    slot_count = boundary.shape[1]
    i32 = jnp.int32
    tail_count = boundary.size + made
    dense = texts * rows == 128 and tail_count == rows and capacity * texts == rows

    qkv_shard, out_shard = attn_qkv.T, attn_out.T
    qkv_fetched = fetch_text(qkv_shard, core)
    out_fetched = fetch_text(out_shard, core)
    qkv_pieces = pieces_of(qkv_shard, qkv_fetched)

    depth = sage_one.shape[0]
    share = depth // texts
    hidden = (graphs // 2) * share
    lanes = next(n for n in range(128, width + 1, 128) if n >= hidden and width % n == 0)
    column = jnp.arange(lanes, dtype=i32)
    wanted = (column // share) * depth + text * share + column % share
    wanted = jnp.where(column < hidden, wanted, -1)
    chosen = (jnp.arange(width, dtype=i32)[:, None] == wanted[None, :]).astype(bf16)
    one_share = dot(sage_one, chosen, ((1,), (0,))).astype(bf16)
    two_share = lax.dynamic_slice_in_dim(sage_two, text * share, share, 0)
    packed = jnp.concatenate(
        [one_share] + [two_share[:, i : i + lanes] for i in range(0, width, lanes)], axis=0
    )
    sage_fetched = fetch_graph(packed)

    tail = jnp.concatenate([boundary.reshape(-1), owner_text.reshape(-1)])
    tail = jnp.pad(tail, (0, -tail_count % rows)).reshape(-1, rows)
    facts = jnp.concatenate([neighbours.T, tail], axis=0).astype(bf16)
    fact_rows = facts.shape[0]
    facts = jnp.pad(facts, ((0, rows - fact_rows), (0, -rows % 128)))
    outset = jnp.concatenate([out_grad, facts], axis=1)
    outset = [outset] + [over_text(outset, k) for k in range(1, texts)]
    shares = swap_cores(sage_fetched)
    normed = layer_norm(tokens, in_gain, in_bias)
    if dense:
        pooled_norm, pooled_context, one, two = attention(
            normed, doc_ids, qkv_pieces, shares, depth, hidden
        )
    else:
        pooled_norm, pooled_context = attention(normed, doc_ids, qkv_pieces, (), depth, hidden)
        one, two = unpack(*shares, depth, share, hidden, width)
    out_fetched, outset, pooled_context = lax.optimization_barrier(
        (out_fetched, outset, pooled_context)
    )
    grads = jnp.concatenate([part[:, :width] for part in outset], axis=0)
    facts = jnp.concatenate([part[:fact_rows, width : width + rows] for part in outset], axis=1)

    def tail_of(facts):
        tail = facts[..., fan:, :].reshape(facts.shape[:-2] + (fact_rows - fan, texts, rows))
        tail = jnp.moveaxis(tail, -2, -3).reshape(facts.shape[:-2] + (texts, -1))
        return tail.astype(i32)

    def slot_places(owners):
        same = owners[..., :, None] == owners[..., None, :]
        order = jnp.arange(made, dtype=i32)
        earlier = jnp.sum((same & (order[None, :] < order[:, None])).astype(i32), axis=-1)
        source = text ^ jnp.arange(texts, dtype=i32)
        place = (owners ^ text) * rows + source[:, None] * capacity + earlier
        return place.reshape(owners.shape[:-2] + (1, texts * made))

    own_places = slot_places(tail_of(facts)[:, tail_count - made : tail_count])
    own_table = (own_places == jnp.arange(texts * rows, dtype=i32)[:, None]).astype(bf16)
    wide = 2 * hidden
    facts_fetched = () if dense else fetch_graph(facts)

    out_pieces = pieces_of(out_shard, out_fetched)
    out_proj = assemble(out_pieces, text, core)
    embedded = dot(pooled_context.astype(bf16), out_proj, ((1,), (1,)))
    embedded = (pooled_norm + embedded).astype(bf16)
    grads, embedded = lax.optimization_barrier((grads, embedded))
    live_grad = dot(own_table, grads, ((0,), (0,))).astype(bf16)
    up = jnp.concatenate(
        [dot(live_grad, two[0], ((1,), (1,))), dot(live_grad, two[1], ((1,), (1,)))], axis=1
    ).astype(bf16)
    if dense:
        up = jnp.concatenate([up, jnp.pad(facts, ((0, 0), (0, wide - facts.shape[1])))])
    up_fetched = fetch_graph(up)
    gathered = jnp.concatenate(
        [embedded] + [over_text(embedded, k) for k in range(1, texts)], axis=0
    )
    first = jnp.concatenate(
        [dot(gathered, one[i], ((1,), (0,)))[:, :hidden] for i in range(2)], axis=1
    ).astype(bf16)
    first_fetched = fetch_graph(first)

    if dense:
        ups = swap_cores(up_fetched)
        links, table = structure(
            *ups, texts, graphs, rows, fan=fan, slot_count=slot_count, made=made
        )
        parts = (*swap_cores(first_fetched), *ups)
        *outgoing, total, live = node_stage_parts((*parts, table, links, one, two), fan)
    else:
        facts = share_cores(facts_fetched)
        ups = share_cores(up_fetched)
        firsts = share_cores(first_fetched)
        listed = facts[:, :fan].reshape(graphs, fan, texts, rows).transpose(0, 2, 3, 1).astype(i32)
        tail = tail_of(facts)
        bounds = tail[..., : tail_count - made].reshape(graphs, texts, graphs, slot_count)
        owners = tail[..., tail_count - made : tail_count]
        places = slot_places(owners)
        peer = graph ^ jnp.arange(graphs, dtype=i32)
        halo_name = (rows + peer[:, None] * slot_count + jnp.arange(slot_count, dtype=i32)).reshape(-1)
        extended_name = jnp.concatenate([jnp.arange(rows, dtype=i32), halo_name])
        turned = (jnp.arange(graphs, dtype=i32)[:, None] == peer[None, :]).astype(f32)
        halo_row = jnp.einsum("ptgk,gd->tdpk", bounds.astype(f32), turned).astype(i32)
        halo_row = halo_row.reshape(texts, graphs, graphs * slot_count)
        halo_at = jnp.repeat(jnp.arange(graphs, dtype=i32), slot_count) * rows + halo_row
        nodes = graphs * rows

        def node_stage(one_text):
            distance, listed, halo_at = one_text
            counts = jnp.sum((listed[..., None] == extended_name).astype(f32), axis=2).astype(bf16)
            table = (places == distance * rows + jnp.arange(rows, dtype=i32)[:, None]).astype(bf16)
            live = jnp.sum(table.astype(f32), axis=2).reshape(nodes, 1)

            def to_rows(by_abstract):
                return dot(table, by_abstract, ((2,), (1,)), ((0,), (0,))).reshape(nodes, -1)

            halo = halo_at.reshape(-1)

            def pull(values, count):
                outer = values[halo].reshape(graphs, -1, values.shape[1])
                inner = values.reshape(graphs, rows, -1)
                extended = jnp.concatenate([inner, outer], axis=1)
                out = dot(counts, extended, ((2,), (1,)), ((0,), (0,)))
                return out.reshape(nodes, -1)[:count]

            def push(values, count):
                out = dot(counts, values.reshape(graphs, rows, -1), ((1,), (1,)), ((0,), (0,)))
                inner = out[:, :rows].reshape(nodes, -1)
                return inner.at[halo].add(out[:, rows:].reshape(halo.shape[0], -1))[:count]

            up_rows = to_rows(ups)
            into_one = up_rows[:, :hidden] + push(up_rows[:, hidden:].astype(bf16), nodes) / fan
            first_rows = to_rows(firsts)
            preact_one = first_rows[:, :hidden] + pull(first_rows[:, hidden:].astype(bf16), nodes) / fan
            gelu_value, pull_back = jax.vjp(jax.nn.gelu, preact_one)
            hidden_one = (live * gelu_value).astype(bf16)
            grad_one = (live * pull_back(into_one)[0]).astype(bf16)
            aggregated = (pull(hidden_one, rows) / fan).astype(bf16)
            returned = (push(grad_one, rows) / fan).astype(bf16)
            return (
                jnp.concatenate([hidden_one[:rows], aggregated], axis=1),
                jnp.concatenate([grad_one[:rows], returned], axis=1),
                live[:rows],
            )

        per_text = (jnp.arange(texts, dtype=i32), listed.transpose(1, 0, 2, 3), halo_at)
        forth, back, live = lax.map(node_stage, per_text)
        forth = forth.reshape(texts * rows, wide)
        state_part = dot(forth[:, :hidden], two[0], ((1,), (0,))) + dot(
            forth[:, hidden:], two[1], ((1,), (0,))
        )
        back = dot(own_table, back.reshape(texts * rows, wide), ((0,), (0,))).astype(bf16)
        grad_part = dot(back[:, :hidden], one[0, :, :hidden], ((1,), (1,))) + dot(
            back[:, hidden:], one[1, :, :hidden], ((1,), (1,))
        )

        final = jnp.concatenate(
            [state_part.reshape(texts, rows, width), grad_part.reshape(texts, made, width)], axis=1
        )
        total, outgoing = final[0], list(final[1:].astype(bf16))
        live = jnp.broadcast_to(live[0], (rows, 128))
    got = [over_text(outgoing[k - 1], k) for k in range(1, texts)]
    return combine(total, live, got)


def solution(mesh):
    rowwise = P(("text", "graph"), None)
    placed = (
        rowwise,
        rowwise,
        P(),
        P(),
        P(None, "text"),
        P(None, "text"),
        rowwise,
        P("graph", None),
        P("graph", None),
        rowwise,
        rowwise,
        rowwise,
    )

    return jax.shard_map(
        local, mesh=mesh, in_specs=placed, out_specs=(rowwise, rowwise), check_vma=False
    )
```

```python
import functools

import jax
import jax.numpy as jnp
from jax import lax
from jax.experimental import pallas as pl
from jax.experimental.pallas import tpu as pltpu
from jax.sharding import PartitionSpec as P

HEAD = 64
SEGS = 4
CORES = 2


epsilon = 1e-06
bf16 = jnp.bfloat16
f32 = jnp.float32


def dot(left, right, contract, batch=((), ())):
    return lax.dot_general(left, right, (contract, batch), preferred_element_type=f32)


def over_text(array, step):
    count = lax.axis_size("text")
    return lax.ppermute(array, "text", [(i, i ^ step) for i in range(count)])


def over_graph(array, step):
    count = lax.axis_size("graph")
    return lax.ppermute(array, "graph", [(i, i ^ step) for i in range(count)])


def over_pair(array, steps):
    texts, graphs = lax.axis_size("text"), lax.axis_size("graph")
    moves = []
    for t in range(texts):
        for g in range(graphs):
            moves.append((t * graphs + g, (t ^ steps[g % CORES]) * graphs + g))
    return lax.ppermute(array, ("text", "graph"), moves)


def natural(parts, own):
    stacked = jnp.stack(parts)
    return jnp.concatenate(
        [lax.dynamic_index_in_dim(stacked, own ^ j, 0, keepdims=True) for j in range(len(parts))]
    )


def fetch_text(shard, core):
    count = lax.axis_size("text")
    half = shard.shape[1] // CORES
    whole = [over_pair(shard, (k, k + 1)) for k in range(1, count - 1, 2)]
    split = lax.dynamic_slice_in_dim(shard, core * half, half, 1)
    return whole + [over_text(split, count - 1)]


def pieces_of(shard, fetched):
    swapped = [over_graph(got, 1) for got in fetched]
    return [shard] + [piece for both in zip(fetched, swapped) for piece in both]


def place_pieces(refs, whole, sem):
    text, core = lax.axis_index("text"), lax.axis_index("graph") % CORES
    rows, width = refs[0].shape
    count = whole.shape[0] // rows
    half = width // CORES
    spots = [(text, 0, width)]
    for k in range(1, count - 1, 2):
        spots += [(text ^ (k + core), 0, width), (text ^ (k + 1 - core), 0, width)]
    spots += [(text ^ (count - 1), core * half, half), (text ^ (count - 1), (1 - core) * half, half)]
    copies = []
    for i, (ref, (peer, lane, lanes)) in enumerate(zip(refs, spots)):
        at = pl.ds(pl.multiple_of(peer * rows, rows), rows)
        if lanes == width:
            target = whole.at[at, :]
        else:
            target = whole.at[at, pl.ds(pl.multiple_of(lane, half), half)]
        copies.append(pltpu.make_async_copy(ref, target, sem.at[i]))
    return copies


def assemble(pieces, text, core):
    parts = [pieces[0]]
    for got, swapped in zip(pieces[1:-2:2], pieces[2:-2:2]):
        parts.append(jnp.where(core == 0, got, swapped))
        parts.append(jnp.where(core == 0, swapped, got))
    got, swapped = pieces[-2:]
    parts.append(
        jnp.concatenate(
            [jnp.where(core == 0, got, swapped), jnp.where(core == 0, swapped, got)], axis=1
        )
    )
    return natural(parts, text).reshape(-1, parts[0].shape[1])


def fetch_graph(array):
    count = lax.axis_size("graph")
    return [array] + [over_graph(array, k) for k in range(CORES, count, CORES)]


def swap_cores(fetched):
    mine = jnp.stack(fetched)
    return mine, over_graph(mine, 1)


def share_cores(fetched):
    both = jnp.stack(swap_cores(fetched), axis=1)
    return both.reshape((-1,) + fetched[0].shape)


def layer_norm(tokens, in_gain, in_bias):
    states = tokens.astype(f32)
    row_mean = jnp.mean(states, axis=1, keepdims=True)
    centred = states - row_mean
    variance = jnp.mean(centred * centred, axis=1, keepdims=True)
    return (centred * lax.rsqrt(variance + epsilon) * in_gain + in_bias).astype(bf16)


def place_shares(mine, swapped, one, two, sem, depth):
    graph = lax.axis_index("graph")
    count, height, lanes = mine.shape
    width = two.shape[2]
    share = (height - depth) * lanes // width
    per_half = CORES * count // 2
    copies = []
    for k in range(count):
        for source, core in ((mine, graph % CORES), (swapped, 1 - graph % CORES)):
            peer = ((graph // CORES) ^ k) * CORES + core
            half, j = peer // per_half, peer % per_half
            at = pl.ds(pl.multiple_of(j * depth, depth), depth)
            moves = [(source.at[k, :depth, :], one.at[half, at, :])]
            at = pl.ds(pl.multiple_of(j * share, share), share)
            for m in range(width // lanes):
                start = depth + m * share
                part = source.at[k, start : start + share, :]
                moves.append((part, two.at[half, at, m * lanes : (m + 1) * lanes]))
            for source_at, target in moves:
                copies.append(pltpu.make_async_copy(source_at, target, sem.at[len(copies)]))
    return copies


def attention_kernel(*refs, pieces, depth):
    normed_ref, doc_ref, doc_column_ref = refs[:3]
    weights, projected, raised, sem, share_sem = refs[-5:]
    copies = place_pieces(refs[3 : 3 + pieces], weights, sem)
    outputs = refs[3 + pieces : -5]
    moves = []
    if depth:
        moves = place_shares(*outputs[:2], *outputs[-2:], share_sem, depth)
        outputs = outputs[2:]
    norm_out, context_out = outputs[:2]
    for copy in copies:
        copy.start()
    for copy in moves:
        copy.start()
    width = normed_ref.shape[1]
    blocks, length = doc_ref.shape
    pair = 2 * HEAD
    lane = lax.broadcasted_iota(jnp.int32, (2 * length, pair), 1)
    row = lax.broadcasted_iota(jnp.int32, (2 * length, pair), 0)
    own_half = (lane < HEAD) == (row < length)
    scale = jnp.where(own_half, HEAD ** (-0.5), 0.0).astype(bf16)
    ones = jnp.ones((2 * SEGS, pair), bf16)
    own_head = (lax.broadcasted_iota(jnp.int32, (4 * SEGS, 2 * length), 0) < 2 * SEGS) == (
        lax.broadcasted_iota(jnp.int32, (4 * SEGS, 2 * length), 1) < length
    )
    members = []
    lengths = []
    for b in range(blocks):
        number = lax.broadcasted_iota(jnp.int32, (2 * SEGS, length), 0)
        member = jnp.where(doc_ref[b : b + 1, :] == number, 1.0, 0.0)
        count = jnp.sum(member, axis=1, keepdims=True)[:SEGS]
        members.append(jnp.concatenate([member, member]))
        lengths.append(count)
        at = slice(b * length, (b + 1) * length)
        pooled = dot(member.astype(bf16), normed_ref[at, :], ((1,), (0,)))
        norm_out[b * SEGS : (b + 1) * SEGS, :] = pooled[:SEGS] / count
    for copy in copies:
        copy.wait()
    step = 2 * pair
    for n in range(0, 3 * width, step):
        out = dot(normed_ref[...], weights[n : n + step, :], ((1,), (1,)))
        projected[:, n : n + step] = out.astype(bf16)
    for b in range(blocks):
        at = slice(b * length, (b + 1) * length)
        same = doc_column_ref[:, b : b + 1] == doc_ref[b : b + 1, :]
        same = jnp.concatenate([same, same])
        starts = range(0, width, pair)
        for i, n in enumerate(starts):
            queries = projected[at, n : n + pair]
            keys = projected[at, width + n : width + n + pair]
            scores = dot(jnp.concatenate([queries, queries]) * scale, keys, ((1,), (1,)))
            raised[i] = jnp.where(same, jnp.exp(scores), 0.0).astype(bf16)
        totals = [dot(ones, raised[i], ((1,), (1,))) for i, n in enumerate(starts)]
        shares = []
        for i, n in enumerate(starts):
            inverse = 1.0 / totals[i]
            inverse = jnp.where(own_head, jnp.concatenate([inverse, inverse]), 0.0)
            high = inverse.astype(bf16)
            low = (inverse - high.astype(f32)).astype(bf16)
            both = dot(jnp.concatenate([high, low]), raised[i], ((1,), (0,)))
            shares.append(both[: 4 * SEGS] + both[4 * SEGS :])
        for i, n in enumerate(starts):
            values = projected[at, 2 * width + n : 2 * width + n + pair]
            mixed = dot((members[b] * shares[i]).astype(bf16), values, ((1,), (0,)))
            both = jnp.where(lane[: 2 * SEGS] < HEAD, mixed[: 2 * SEGS], mixed[2 * SEGS :])
            context_out[b * SEGS : (b + 1) * SEGS, n : n + pair] = both[:SEGS] / lengths[b]
    for copy in moves:
        copy.wait()


def attention(normed, doc_ids, pieces, shares, depth, hidden):
    tokens, width = normed.shape
    blocks, length = doc_ids.shape
    vmem, anywhere = pl.BlockSpec(memory_space=pltpu.VMEM), pl.BlockSpec(memory_space=pl.ANY)
    pooled = jax.ShapeDtypeStruct((blocks * SEGS, width), f32)
    placed, moves = (), 1
    if shares:
        count, _, lanes = shares[0].shape
        placed = (
            jax.ShapeDtypeStruct((2, width, lanes), bf16),
            jax.ShapeDtypeStruct((2, hidden, width), bf16),
        )
        moves = CORES * count * (1 + width // lanes)
    flops = 2 * tokens * width * 3 * width + 6 * tokens * length * width
    return pl.pallas_call(
        functools.partial(attention_kernel, pieces=len(pieces), depth=depth if shares else 0),
        out_shape=(pooled, pooled) + placed,
        in_specs=[vmem] * 3 + [anywhere] * (len(pieces) + len(shares)),
        out_specs=(vmem,) * (2 + len(placed)),
        scratch_shapes=[
            pltpu.VMEM((3 * width, width), bf16),
            pltpu.VMEM((tokens, 3 * width), bf16),
            pltpu.VMEM((width // (2 * HEAD), 2 * length, length), bf16),
            pltpu.SemaphoreType.DMA((len(pieces),)),
            pltpu.SemaphoreType.DMA((moves,)),
        ],
        cost_estimate=pl.CostEstimate(
            flops=flops, bytes_accessed=8 * width * width, transcendentals=tokens * length * width // HEAD
        ),
        name="attention",
    )(normed, doc_ids, doc_ids.T, *pieces, *shares)


def structure_kernel(mine, swapped, links, table, *, fan, slot_count, made):
    texts, nodes, _ = links.shape
    graphs = table.shape[0]
    rows = nodes // graphs
    lanes = texts * rows
    capacity = rows // texts
    text, graph = lax.axis_index("text"), lax.axis_index("graph")
    skip = texts * made
    facts = [
        (swapped if d % CORES else mine)[d // CORES, skip:, :lanes].astype(f32)
        for d in range(graphs)
    ]
    tails = jnp.concatenate([each[fan : fan + 1] for each in facts]).astype(jnp.int32)
    lane = lax.broadcasted_iota(jnp.int32, (graphs, lanes), 1)

    owner_at = graphs * slot_count
    own = lane % rows - owner_at
    earlier = jnp.zeros_like(tails)
    for j in range(1, made):
        earlier += jnp.where((own >= j) & (pltpu.roll(tails, j, 1) == tails), 1, 0)
    place = (tails ^ text) * rows + (text ^ (lane // rows)) * capacity + earlier
    place = jnp.concatenate(
        [place[:, t * rows + owner_at : t * rows + owner_at + made] for t in range(texts)], axis=1
    )
    row = lax.broadcasted_iota(jnp.int32, (lanes, texts * made), 0)
    for d in range(graphs):
        table[d] = jnp.where(row == place[d : d + 1], 1.0, 0.0).astype(bf16)

    turned = tails
    bit = 1
    while bit < graphs:
        step = bit * slot_count
        up, down = pltpu.roll(turned, step, 1), pltpu.roll(turned, lanes - step, 1)
        moved = jnp.where((lane // slot_count) & bit != 0, up, down)
        turned = jnp.where(graph & bit != 0, moved, turned)
        bit *= 2
    entry = lax.broadcasted_iota(jnp.int32, (rows + owner_at, lanes), 0)
    outer = entry - rows
    name = rows + (graph ^ (outer % graphs)) * slot_count + outer // graphs
    name = jnp.where(entry < rows, entry, name).astype(f32)
    column = lax.broadcasted_iota(jnp.int32, (rows, nodes), 1)
    inner = lax.broadcasted_iota(jnp.int32, (rows, nodes), 0)
    base = lax.broadcasted_iota(jnp.int32, (graphs, nodes), 0) * rows
    for d in range(graphs):
        counts = jnp.zeros((rows + owner_at, lanes), f32)
        for f in range(fan):
            counts += jnp.where(facts[d][f : f + 1] == name, 1.0, 0.0)
        counts = counts.T.astype(bf16)
        for t in range(texts):
            spots = [jnp.where(column == inner + d * rows, 1.0, 0.0)]
            for k in range(slot_count):
                at = t * rows + d * slot_count + k
                target = base + turned[:, at : at + 1]
                spots.append(jnp.where(column[:graphs] == target, 1.0, 0.0))
            spots = jnp.concatenate(spots).astype(bf16)
            linked = dot(counts[t * rows : (t + 1) * rows], spots, ((1,), (0,)))
            links[t, d * rows : (d + 1) * rows, :] = linked.astype(bf16)


def node_kernel(mine, swapped, up_mine, up_swapped, table, links, one, two, *refs, fan):
    first_self, first_next, up_self, up_next, live, kept = refs[-6:]
    own, live_out = refs[-8:-6]
    texts, nodes, _ = links.shape
    graphs = table.shape[0]
    rows = nodes // graphs
    made = table.shape[2] // texts
    hidden = two.shape[1]
    ones = jnp.ones((texts * made, live.shape[2]), bf16)
    for d in range(graphs):
        chosen = table[d]
        values = (swapped if d % CORES else mine)[d // CORES]
        ups = (up_swapped if d % CORES else up_mine)[d // CORES, : texts * made]
        for target, value in (
            (live, ones),
            (first_self, values[:, :hidden]),
            (first_next, values[:, hidden:]),
            (up_self, ups[:, :hidden]),
            (up_next, ups[:, hidden:]),
        ):
            placed = dot(chosen, value, ((1,), (0,))).astype(bf16)
            for t in range(texts):
                target[t, d * rows : (d + 1) * rows, :] = placed[t * rows : (t + 1) * rows]
    for t in range(texts):
        linked = links[t]
        x = first_self[t].astype(f32) + dot(linked, first_next[t], ((1,), (0,))) / fan
        into = up_self[t].astype(f32) + dot(linked, up_next[t], ((0,), (0,))) / fan
        alive = live[t][:, :1].astype(f32)
        square = x * x
        slope = 0.7978845608028654 * (1.0 + 3.0 * 0.044715 * square)
        half = 0.5 * (1.0 + jnp.tanh(0.7978845608028654 * (x + 0.044715 * square * x)))
        value = (alive * (x * half)).astype(bf16)
        grad = (alive * ((half + 2.0 * x * half * (1.0 - half) * slope) * into)).astype(bf16)
        at = slice(t * rows, (t + 1) * rows)
        kept[0, at, :] = value[:rows]
        kept[1, at, :] = (dot(linked[:rows], value, ((1,), (0,))) / fan).astype(bf16)
        kept[2, at, :] = grad[:rows]
        kept[3, at, :] = (dot(linked[:, :rows], grad, ((0,), (0,))) / fan).astype(bf16)
    state = dot(kept[0], two[0], ((1,), (0,))) + dot(kept[1], two[1], ((1,), (0,)))
    back = [dot(table[0], kept[i], ((0,), (0,))).astype(bf16) for i in (2, 3)]
    returned = dot(back[0], one[0, :, :hidden], ((1,), (1,))) + dot(
        back[1], one[1, :, :hidden], ((1,), (1,))
    )
    for t in range(1, texts):
        refs[t - 1][:rows, :] = state[t * rows : (t + 1) * rows].astype(bf16)
        refs[t - 1][rows:, :] = returned[t * made : (t + 1) * made].astype(bf16)
    own[:rows, :] = state[:rows]
    own[rows:, :] = returned[:made]
    live_out[...] = live[0, :rows, :].astype(f32)


def unpack_kernel(mine, swapped, one, two, *, depth, share):
    graph = lax.axis_index("graph")
    graphs = CORES * mine.shape[0]
    width = two.shape[2]
    lanes = mine.shape[2]
    same = graph % CORES == 0
    for g in range(graphs):
        z = (graph // CORES) ^ (g // CORES)
        near, far = mine[z], swapped[z]
        got = jnp.where(same == (g % CORES == 0), near, far)
        half, j = g // (graphs // 2), g % (graphs // 2)
        one[half, j * depth : (j + 1) * depth, :] = got[:depth]
        for m in range(width // lanes):
            part = got[depth + m * share : depth + (m + 1) * share]
            two[half, j * share : (j + 1) * share, m * lanes : (m + 1) * lanes] = part


def unpack(mine, swapped, depth, share, hidden, width):
    vmem = pl.BlockSpec(memory_space=pltpu.VMEM)
    return pl.pallas_call(
        functools.partial(unpack_kernel, depth=depth, share=share),
        out_shape=(
            jax.ShapeDtypeStruct((2, width, mine.shape[2]), bf16),
            jax.ShapeDtypeStruct((2, hidden, width), bf16),
        ),
        in_specs=[vmem] * 2,
        out_specs=(vmem, vmem),
        cost_estimate=pl.CostEstimate(flops=10**8, bytes_accessed=10**6, transcendentals=0),
        name="unpack",
    )(mine, swapped)


def structure(mine, swapped, texts, graphs, rows, **sizes):
    vmem = pl.BlockSpec(memory_space=pltpu.VMEM)
    nodes, made = graphs * rows, sizes["made"]
    return pl.pallas_call(
        functools.partial(structure_kernel, **sizes),
        out_shape=(
            jax.ShapeDtypeStruct((texts, nodes, nodes), bf16),
            jax.ShapeDtypeStruct((graphs, texts * rows, texts * made), bf16),
        ),
        in_specs=[vmem] * 2,
        out_specs=(vmem, vmem),
        cost_estimate=pl.CostEstimate(flops=10**9, bytes_accessed=10**6, transcendentals=0),
        name="structure",
    )(mine, swapped)


def node_stage_parts(arrays, fan):
    vmem = pl.BlockSpec(memory_space=pltpu.VMEM)
    table, links, _, two = arrays[4:]
    texts, nodes, _ = links.shape
    rows = nodes // table.shape[0]
    made = table.shape[2] // texts
    hidden, width = two.shape[1:]
    return pl.pallas_call(
        functools.partial(node_kernel, fan=fan),
        out_shape=[jax.ShapeDtypeStruct((rows + made, width), bf16)] * (texts - 1)
        + [
            jax.ShapeDtypeStruct((rows + made, width), f32),
            jax.ShapeDtypeStruct((rows, 128), f32),
        ],
        in_specs=[vmem] * len(arrays),
        out_specs=[vmem] * (texts + 1),
        scratch_shapes=[pltpu.VMEM((texts, nodes, hidden), bf16)] * 4
        + [pltpu.VMEM((texts, nodes, 128), bf16), pltpu.VMEM((4, texts * rows, hidden), bf16)],
        cost_estimate=pl.CostEstimate(flops=10**9, bytes_accessed=10**6, transcendentals=10**6),
        name="nodes",
    )(*arrays)


def combine_kernel(own, live, *refs):
    states, grads = refs[-2:]
    rows = states.shape[0]
    total = own[...]
    for part in refs[:-2]:
        total += part[...].astype(f32)
    states[...] = (live[:, :1] * total[:rows]).astype(bf16)
    grads[...] = total[rows:].astype(bf16)


def combine(own, live, got):
    vmem = pl.BlockSpec(memory_space=pltpu.VMEM)
    rows, width = live.shape[0], own.shape[1]
    return pl.pallas_call(
        combine_kernel,
        out_shape=(
            jax.ShapeDtypeStruct((rows, width), bf16),
            jax.ShapeDtypeStruct((own.shape[0] - rows, width), bf16),
        ),
        in_specs=[vmem] * (2 + len(got)),
        out_specs=(vmem, vmem),
        name="combine",
    )(own, live, *got)


def local(
    tokens,
    doc_ids,
    in_gain,
    in_bias,
    attn_qkv,
    attn_out,
    owner_text,
    sage_one,
    sage_two,
    neighbours,
    boundary,
    out_grad,
):
    width = tokens.shape[1]
    texts, graphs = lax.axis_size("text"), lax.axis_size("graph")
    text, graph = lax.axis_index("text"), lax.axis_index("graph")
    core = graph % CORES
    rows = out_grad.shape[0]
    made = owner_text.shape[0]
    capacity = rows // texts
    fan = neighbours.shape[1]
    slot_count = boundary.shape[1]
    i32 = jnp.int32
    tail_count = boundary.size + made
    dense = texts * rows == 128 and tail_count == rows and capacity * texts == rows

    qkv_shard, out_shard = attn_qkv.T, attn_out.T
    qkv_fetched = fetch_text(qkv_shard, core)
    out_fetched = fetch_text(out_shard, core)
    qkv_pieces = pieces_of(qkv_shard, qkv_fetched)

    depth = sage_one.shape[0]
    share = depth // texts
    hidden = (graphs // 2) * share
    lanes = next(n for n in range(128, width + 1, 128) if n >= hidden and width % n == 0)
    column = jnp.arange(lanes, dtype=i32)
    wanted = (column // share) * depth + text * share + column % share
    wanted = jnp.where(column < hidden, wanted, -1)
    chosen = (jnp.arange(width, dtype=i32)[:, None] == wanted[None, :]).astype(bf16)
    one_share = dot(sage_one, chosen, ((1,), (0,))).astype(bf16)
    two_share = lax.dynamic_slice_in_dim(sage_two, text * share, share, 0)
    packed = jnp.concatenate(
        [one_share] + [two_share[:, i : i + lanes] for i in range(0, width, lanes)], axis=0
    )
    sage_fetched = fetch_graph(packed)

    tail = jnp.concatenate([boundary.reshape(-1), owner_text.reshape(-1)])
    tail = jnp.pad(tail, (0, -tail_count % rows)).reshape(-1, rows)
    facts = jnp.concatenate([neighbours.T, tail], axis=0).astype(bf16)
    fact_rows = facts.shape[0]
    facts = jnp.pad(facts, ((0, rows - fact_rows), (0, -rows % 128)))
    outset = jnp.concatenate([out_grad, facts], axis=1)
    outset = [outset] + [over_text(outset, k) for k in range(1, texts)]
    shares = swap_cores(sage_fetched)
    normed = layer_norm(tokens, in_gain, in_bias)
    if dense:
        pooled_norm, pooled_context, one, two = attention(
            normed, doc_ids, qkv_pieces, shares, depth, hidden
        )
    else:
        pooled_norm, pooled_context = attention(normed, doc_ids, qkv_pieces, (), depth, hidden)
        one, two = unpack(*shares, depth, share, hidden, width)
    out_fetched, pooled_context = lax.optimization_barrier((out_fetched, pooled_context))
    grads = jnp.concatenate([part[:, :width] for part in outset], axis=0)
    facts = [part[:fact_rows, width : width + rows] for part in outset]
    facts = jnp.concatenate(facts, axis=1)

    def tail_of(facts):
        tail = facts[..., fan:, :].reshape(facts.shape[:-2] + (fact_rows - fan, texts, rows))
        tail = jnp.moveaxis(tail, -2, -3).reshape(facts.shape[:-2] + (texts, -1))
        return tail.astype(i32)

    def slot_places(owners):
        same = owners[..., :, None] == owners[..., None, :]
        order = jnp.arange(made, dtype=i32)
        earlier = jnp.sum((same & (order[None, :] < order[:, None])).astype(i32), axis=-1)
        source = text ^ jnp.arange(texts, dtype=i32)
        place = (owners ^ text) * rows + source[:, None] * capacity + earlier
        return place.reshape(owners.shape[:-2] + (1, texts * made))

    own_places = slot_places(tail_of(facts)[:, tail_count - made : tail_count])
    own_table = (own_places == jnp.arange(texts * rows, dtype=i32)[:, None]).astype(bf16)
    wide = 2 * hidden
    facts_fetched = () if dense else fetch_graph(facts)

    out_pieces = pieces_of(out_shard, out_fetched)
    out_proj = assemble(out_pieces, text, core)
    embedded = dot(pooled_context.astype(bf16), out_proj, ((1,), (1,)))
    embedded = (pooled_norm + embedded).astype(bf16)
    grads, embedded = lax.optimization_barrier((grads, embedded))
    live_grad = dot(own_table, grads, ((0,), (0,))).astype(bf16)
    up = jnp.concatenate(
        [dot(live_grad, two[0], ((1,), (1,))), dot(live_grad, two[1], ((1,), (1,)))], axis=1
    ).astype(bf16)
    if dense:
        up = jnp.concatenate([up, jnp.pad(facts, ((0, 0), (0, wide - facts.shape[1])))])
    up_fetched = fetch_graph(up)
    gathered = jnp.concatenate(
        [embedded] + [over_text(embedded, k) for k in range(1, texts)], axis=0
    )
    first = dot(gathered, one, ((1,), (1,)))[:, :, :hidden].reshape(-1, wide).astype(bf16)
    first_fetched = fetch_graph(first)

    if dense:
        ups = swap_cores(up_fetched)
        links, table = structure(
            *ups, texts, graphs, rows, fan=fan, slot_count=slot_count, made=made
        )
        parts = (*swap_cores(first_fetched), *ups)
        *outgoing, total, live = node_stage_parts((*parts, table, links, one, two), fan)
    else:
        facts = share_cores(facts_fetched)
        ups = share_cores(up_fetched)
        firsts = share_cores(first_fetched)
        listed = facts[:, :fan].reshape(graphs, fan, texts, rows).transpose(0, 2, 3, 1).astype(i32)
        tail = tail_of(facts)
        bounds = tail[..., : tail_count - made].reshape(graphs, texts, graphs, slot_count)
        owners = tail[..., tail_count - made : tail_count]
        places = slot_places(owners)
        peer = graph ^ jnp.arange(graphs, dtype=i32)
        halo_name = (rows + peer[:, None] * slot_count + jnp.arange(slot_count, dtype=i32)).reshape(-1)
        extended_name = jnp.concatenate([jnp.arange(rows, dtype=i32), halo_name])
        turned = (jnp.arange(graphs, dtype=i32)[:, None] == peer[None, :]).astype(f32)
        halo_row = jnp.einsum("ptgk,gd->tdpk", bounds.astype(f32), turned).astype(i32)
        halo_row = halo_row.reshape(texts, graphs, graphs * slot_count)
        halo_at = jnp.repeat(jnp.arange(graphs, dtype=i32), slot_count) * rows + halo_row
        nodes = graphs * rows

        def node_stage(one_text):
            distance, listed, halo_at = one_text
            counts = jnp.sum((listed[..., None] == extended_name).astype(f32), axis=2).astype(bf16)
            table = (places == distance * rows + jnp.arange(rows, dtype=i32)[:, None]).astype(bf16)
            live = jnp.sum(table.astype(f32), axis=2).reshape(nodes, 1)

            def to_rows(by_abstract):
                return dot(table, by_abstract, ((2,), (1,)), ((0,), (0,))).reshape(nodes, -1)

            halo = halo_at.reshape(-1)

            def pull(values, count):
                outer = values[halo].reshape(graphs, -1, values.shape[1])
                inner = values.reshape(graphs, rows, -1)
                extended = jnp.concatenate([inner, outer], axis=1)
                out = dot(counts, extended, ((2,), (1,)), ((0,), (0,)))
                return out.reshape(nodes, -1)[:count]

            def push(values, count):
                out = dot(counts, values.reshape(graphs, rows, -1), ((1,), (1,)), ((0,), (0,)))
                inner = out[:, :rows].reshape(nodes, -1)
                return inner.at[halo].add(out[:, rows:].reshape(halo.shape[0], -1))[:count]

            up_rows = to_rows(ups)
            into_one = up_rows[:, :hidden] + push(up_rows[:, hidden:].astype(bf16), nodes) / fan
            first_rows = to_rows(firsts)
            preact_one = first_rows[:, :hidden] + pull(first_rows[:, hidden:].astype(bf16), nodes) / fan
            gelu_value, pull_back = jax.vjp(jax.nn.gelu, preact_one)
            hidden_one = (live * gelu_value).astype(bf16)
            grad_one = (live * pull_back(into_one)[0]).astype(bf16)
            aggregated = (pull(hidden_one, rows) / fan).astype(bf16)
            returned = (push(grad_one, rows) / fan).astype(bf16)
            return (
                jnp.concatenate([hidden_one[:rows], aggregated], axis=1),
                jnp.concatenate([grad_one[:rows], returned], axis=1),
                live[:rows],
            )

        per_text = (jnp.arange(texts, dtype=i32), listed.transpose(1, 0, 2, 3), halo_at)
        forth, back, live = lax.map(node_stage, per_text)
        forth = forth.reshape(texts * rows, wide)
        state_part = dot(forth[:, :hidden], two[0], ((1,), (0,))) + dot(
            forth[:, hidden:], two[1], ((1,), (0,))
        )
        back = dot(own_table, back.reshape(texts * rows, wide), ((0,), (0,))).astype(bf16)
        grad_part = dot(back[:, :hidden], one[0, :, :hidden], ((1,), (1,))) + dot(
            back[:, hidden:], one[1, :, :hidden], ((1,), (1,))
        )

        final = jnp.concatenate(
            [state_part.reshape(texts, rows, width), grad_part.reshape(texts, made, width)], axis=1
        )
        total, outgoing = final[0], list(final[1:].astype(bf16))
        live = jnp.broadcast_to(live[0], (rows, 128))
    got = [over_text(outgoing[k - 1], k) for k in range(1, texts)]
    return combine(total, live, got)


def solution(mesh):
    rowwise = P(("text", "graph"), None)
    placed = (
        rowwise,
        rowwise,
        P(),
        P(),
        P(None, "text"),
        P(None, "text"),
        rowwise,
        P("graph", None),
        P("graph", None),
        rowwise,
        rowwise,
        rowwise,
    )

    return jax.shard_map(
        local, mesh=mesh, in_specs=placed, out_specs=(rowwise, rowwise), check_vma=False
    )
```
